8 devices in a mesh: side: 2 (over z, y), rep: 4 (over x, core).
Axes of the slice: x: 2, y: 2, z: 1, core: 2. Of those that a mesh axis runs over, the one named last changes fastest.
Arguments:
- w_up: float32 [2, 1, 2048, 8192], P('side', None, 'rep')
- w_down: float32 [2, 1, 8192, 2048], P('side', None, None, 'rep')
- g_up: float32 [2, 1, 2048, 8192], P('side', None, 'rep')
- g_down: float32 [2, 1, 8192, 2048], P('side', None, None, 'rep')
- learn_rate: float32 [1], replicated
- old_up: bfloat16 [2, 4, 1, 2048, 8192], P('side', 'rep')
- old_down: bfloat16 [2, 4, 1, 8192, 2048], P('side', 'rep')
- prompts: bfloat16 [2, 4, 2048, 2048], P('side', 'rep')
Outputs:
- output 1: float32 [2, 1, 2048, 8192], P('side', None, 'rep')
- output 2: float32 [2, 1, 8192, 2048], P('side', None, None, 'rep')
- output 3: bfloat16 [2, 4, 2048, 2048], P('side', 'rep')
All inputs are finite; a program needn't handle non-finite values.
Results may differ from the reference program's by a relative error of at most 0.001.
Values are sent between devices in bfloat16 or wider.
A program may use at most 1 GiB of HBM per device.

```python
import jax
import jax.numpy as jnp
from jax import lax

MODEL_DIM = 2048
HIDDEN_DIM = 8192
LAYERS = 1
TOKENS = 2048
REPLICAS = 4
TP_WIDTH = 1
SHARD_DIM = HIDDEN_DIM // TP_WIDTH


def split_up(full):
    return jnp.transpose(full.reshape(LAYERS, MODEL_DIM, TP_WIDTH, SHARD_DIM), (2, 0, 1, 3))


def split_down(full):
    return jnp.transpose(full.reshape(LAYERS, TP_WIDTH, SHARD_DIM, MODEL_DIM), (1, 0, 2, 3))


def merge_up(blocks):
    return jnp.transpose(blocks, (1, 2, 0, 3)).reshape(LAYERS, MODEL_DIM, HIDDEN_DIM)


def merge_down(blocks):
    return jnp.transpose(blocks, (1, 0, 2, 3)).reshape(LAYERS, HIDDEN_DIM, MODEL_DIM)


def trainer_slots(blocks):
    return jnp.concatenate([blocks, jnp.zeros_like(blocks)], axis=0)


def generator_slots(blocks):
    copies = jnp.broadcast_to(blocks[:, None], (TP_WIDTH, REPLICAS) + blocks.shape[1:])
    return jnp.concatenate([jnp.zeros_like(copies), copies], axis=0)


def setup_inputs(seed: int = 0) -> dict:
    rng_keys = jax.random.split(jax.random.key(seed), 8)
    up_scale = MODEL_DIM ** -0.5
    down_scale = HIDDEN_DIM ** -0.5
    up_shape = (LAYERS, MODEL_DIM, HIDDEN_DIM)
    down_shape = (LAYERS, HIDDEN_DIM, MODEL_DIM)
    w_up_full = jax.random.normal(rng_keys[0], up_shape, jnp.float32) * up_scale
    w_down_full = jax.random.normal(rng_keys[1], down_shape, jnp.float32) * down_scale
    g_up_full = jax.random.normal(rng_keys[2], up_shape, jnp.float32) * up_scale
    g_down_full = jax.random.normal(rng_keys[3], down_shape, jnp.float32) * down_scale
    learn_rate = jax.random.uniform(rng_keys[4], (1,), jnp.float32, minval=0.15, maxval=0.3)
    stale_up = (w_up_full + 0.2 * up_scale * jax.random.normal(rng_keys[5], up_shape, jnp.float32)).astype(jnp.bfloat16)
    stale_down = (w_down_full + 0.2 * down_scale * jax.random.normal(rng_keys[6], down_shape, jnp.float32)).astype(jnp.bfloat16)
    prompt_rows = jax.random.normal(rng_keys[7], (REPLICAS, TOKENS, MODEL_DIM), jnp.float32).astype(jnp.bfloat16)
    prompt_copies = jnp.broadcast_to(prompt_rows[None], (TP_WIDTH,) + prompt_rows.shape)
    return {
        "w_up": trainer_slots(split_up(w_up_full)),
        "w_down": trainer_slots(split_down(w_down_full)),
        "g_up": trainer_slots(split_up(g_up_full)),
        "g_down": trainer_slots(split_down(g_down_full)),
        "learn_rate": learn_rate,
        "old_up": generator_slots(split_up(stale_up)),
        "old_down": generator_slots(split_down(stale_down)),
        "prompts": jnp.concatenate([jnp.zeros_like(prompt_copies), prompt_copies], axis=0),
    }


def layer_step(hidden, weights):
    up_mat, down_mat = weights
    pre_act = jnp.dot(hidden, up_mat, preferred_element_type=jnp.float32)
    act_val = jax.nn.gelu(pre_act, approximate=False).astype(jnp.bfloat16)
    branch = jnp.dot(act_val, down_mat, preferred_element_type=jnp.float32)
    return (hidden.astype(jnp.float32) + branch).astype(jnp.bfloat16), None


def reference(w_up, w_down, g_up, g_down, learn_rate, old_up, old_down, prompts):
    step_rate = learn_rate[0]
    new_up = w_up - step_rate * g_up
    new_down = w_down - step_rate * g_down
    delta_up = merge_up((new_up - w_up)[:TP_WIDTH].astype(jnp.bfloat16)).astype(jnp.float32)
    delta_down = merge_down((new_down - w_down)[:TP_WIDTH].astype(jnp.bfloat16)).astype(jnp.float32)
    stale_gen_up = jnp.swapaxes(old_up[TP_WIDTH:], 0, 1)
    stale_gen_down = jnp.swapaxes(old_down[TP_WIDTH:], 0, 1)

    def one_replica(operands):
        rep_up, rep_down, rep_x = operands
        gen_up = (merge_up(rep_up).astype(jnp.float32) + delta_up).astype(jnp.bfloat16)
        gen_down = (merge_down(rep_down).astype(jnp.float32) + delta_down).astype(jnp.bfloat16)
        final_h, _ = lax.scan(layer_step, rep_x, (gen_up, gen_down))
        return final_h

    gen_out = lax.map(one_replica, (stale_gen_up, stale_gen_down, prompts[TP_WIDTH]))
    gen_copies = jnp.broadcast_to(gen_out[None], (TP_WIDTH,) + gen_out.shape)
    outputs = jnp.concatenate([jnp.zeros_like(gen_copies), gen_copies], axis=0)
    return new_up, new_down, outputs
```

```python
import functools

import jax
import jax.numpy as jnp
from jax import lax
from jax.experimental import pallas as pl
from jax.experimental.pallas import tpu as pltpu
from jax.sharding import PartitionSpec as P

MESH = pl.DeviceIdType.MESH
COLS = 256
SENDS = 4
TILE = 512


def gelu(x):
    return 0.5 * x * (1.0 + lax.erf(x * 0.7071067811865476))


def sync_kernel(lr, w_up, w_dn, g_up, g_dn, s_up, s_dn, x_hbm, y_hbm, land_up, land_dn,
                wb_up, wb_dn, gb_up, gb_dn, d_up, d_dn,
                x_v, acc, sb_up, sb_dn, lb_up, lb_dn, wg_up, wg_dn, u_v,
                t_sem, send_sem, s_sem, l_sem, x_sem, y_recv, x_recv, o_recv, n_recv, x_send, o_send, n_send):
    side, rep = lax.axis_index("side"), lax.axis_index("rep")
    other = 1 - side
    sib = rep + 1 - 2 * (rep % 2)
    cross = (rep + 2) % 4
    chunks = land_up.shape[0]
    depth = w_up.shape[0]
    lands, smalls = (land_up, land_dn), (d_up, d_dn)

    barrier = pltpu.get_barrier_semaphore()
    for dev in ((other, rep), (side, sib), (side, cross)):
        pl.semaphore_signal(barrier, inc=1, device_id=dev, device_id_type=MESH)
    pl.semaphore_wait(barrier, 3)

    def span(m):
        return pl.ds(pl.multiple_of(m * COLS, COLS), COLS)

    @pl.when(side == 0)
    def trainer():
        def loads(m):
            k = m % 2
            return [
                pltpu.make_async_copy(w_up.at[:, span(m)], wb_up.at[k], t_sem.at[0, k]),
                pltpu.make_async_copy(g_up.at[:, span(m)], gb_up.at[k], t_sem.at[1, k]),
                pltpu.make_async_copy(w_dn.at[span(m), :], wb_dn.at[k], t_sem.at[2, k]),
                pltpu.make_async_copy(g_dn.at[span(m), :], gb_dn.at[k], t_sem.at[3, k]),
            ]

        def send(h, m):
            return pltpu.make_async_remote_copy(
                src_ref=smalls[h].at[m % SENDS], dst_ref=lands[h].at[m, rep],
                send_sem=send_sem.at[h, m % SENDS], recv_sem=y_recv.at[h, m],
                device_id=(other, rep), device_id_type=MESH)

        for m in range(2):
            for c in loads(m):
                c.start()
        rate = lr[0]

        def step(m, _):
            k = m % 2
            for c in loads(m):
                c.wait()

            @pl.when(m >= SENDS)
            def _():
                for h in range(2):
                    send(h, m - SENDS).wait_send()

            for w, g, d in ((wb_up, gb_up, d_up), (wb_dn, gb_dn, d_dn)):
                old = w[k]
                d[m % SENDS] = ((old - rate * g[k]) - old).astype(jnp.bfloat16)

            @pl.when(m + 2 < chunks)
            def _():
                for c in loads(m + 2):
                    c.start()

            @pl.when(m >= 1)
            def _():
                for h in range(2):
                    send(h, m - 1).start()
            return 0

        lax.fori_loop(0, chunks, step, 0)
        for h in range(2):
            send(h, chunks - 1).start()
        for m in range(chunks - SENDS, chunks):
            for h in range(2):
                send(h, m).wait_send()

    @pl.when(side == 1)
    def generator():
        def hop(h, m, row, dev, send, recv):
            return pltpu.make_async_remote_copy(
                src_ref=lands[h].at[m, row], dst_ref=lands[h].at[m, row],
                send_sem=send.at[h, m], recv_sem=recv.at[h, m],
                device_id=(side, dev), device_id_type=MESH)

        def from_trainer(h, m):
            return hop(h, m, rep, sib, x_send, y_recv)

        def across(h, m, row):
            return hop(h, m, row, cross, x_send, x_recv)

        def own(h, m, row):
            return hop(h, m, row, sib, o_send, o_recv)

        def next_own(h, m, row):
            return hop(h, m, row, sib, n_send, n_recv)

        sib_cross = (sib + 2) % 4
        stales = ((s_up, sb_up), (s_dn, sb_dn))

        def stale(h, m):
            src = s_up.at[:, span(m)] if h == 0 else s_dn.at[span(m), :]
            return pltpu.make_async_copy(src, stales[h][1].at[m % 2], s_sem.at[h, m % 2])

        def landed(h, m):
            return pltpu.make_async_copy(lands[h].at[m], (lb_up, lb_dn)[h].at[m % 2], l_sem.at[h, m % 2])

        x_in = pltpu.make_async_copy(x_hbm, x_v, x_sem.at[0])
        x_in.start()
        for m in range(2):
            for h in range(2):
                stale(h, m).start()
        acc[...] = jnp.zeros_like(acc)
        x_in.wait()

        def route(h, m):
            @pl.when(m < chunks)
            def _():
                from_trainer(h, m).wait_recv()
                across(h, m, rep).start()
                own(h, m, rep).start()

            @pl.when((m >= 1) & (m < chunks + 1))
            def _():
                across(h, m - 1, cross).wait_recv()
                next_own(h, m - 1, cross).start()

            @pl.when((m >= 2) & (m < chunks + 2))
            def _():
                own(h, m - 2, sib).wait_recv()
                next_own(h, m - 2, sib_cross).wait_recv()
                landed(h, m - 2).start()

        def up(m):
            k = m % 2
            landed(0, m).wait()
            stale(0, m).wait()
            for r in range(4):
                rows = pl.ds(r * depth, depth)
                wg_up[rows, :] = (sb_up[k, rows, :].astype(jnp.float32) + lb_up[k, r].astype(jnp.float32)).astype(jnp.bfloat16)

            @pl.when(m + 2 < chunks)
            def _():
                stale(0, m + 2).start()

            def tile(i, _):
                rows = pl.ds(pl.multiple_of(i * TILE, TILE), TILE)
                pre = jnp.dot(x_v[rows, :], wg_up[...], preferred_element_type=jnp.float32)
                u_v[rows, :] = gelu(pre).astype(jnp.bfloat16)
                return 0
            lax.fori_loop(0, x_v.shape[0] // TILE, tile, 0)

        def down(m):
            k = m % 2
            landed(1, m).wait()
            stale(1, m).wait()
            for r in range(4):
                cols = pl.ds(r * depth, depth)
                wg_dn[:, cols] = (sb_dn[k, :, cols].astype(jnp.float32) + lb_dn[k, r].astype(jnp.float32)).astype(jnp.bfloat16)

            @pl.when(m + 2 < chunks)
            def _():
                stale(1, m + 2).start()

            def tile(i, _):
                rows = pl.ds(pl.multiple_of(i * TILE, TILE), TILE)
                acc[rows, :] += jnp.dot(u_v[rows, :], wg_dn[...], preferred_element_type=jnp.float32)
                return 0
            lax.fori_loop(0, x_v.shape[0] // TILE, tile, 0)

        def step(m, _):
            route(0, m)

            @pl.when(m >= 3)
            def _():
                down(m - 3)
            route(1, m)

            @pl.when((m >= 2) & (m < chunks + 2))
            def _():
                up(m - 2)
            return 0

        lax.fori_loop(0, chunks + 3, step, 0)

        def finish(i, _):
            rows = pl.ds(pl.multiple_of(i * TILE, TILE), TILE)
            x_v[rows, :] = (x_v[rows, :].astype(jnp.float32) + acc[rows, :]).astype(jnp.bfloat16)
            return 0
        lax.fori_loop(0, x_v.shape[0] // TILE, finish, 0)
        out = pltpu.make_async_copy(x_v, y_hbm, x_sem.at[0])
        out.start()

        def drain(m, _):
            for h in range(2):
                across(h, m, rep).wait_send()
                own(h, m, rep).wait_send()
                next_own(h, m, cross).wait_send()
            return 0
        lax.fori_loop(0, chunks, drain, 0)
        out.wait()


def synced_output(lr, w_up, w_dn, g_up, g_dn, s_up, s_dn, x):
    depth, hid = w_up.shape
    tokens, width = x.shape
    chunks = hid // COLS
    any_spec = pl.BlockSpec(memory_space=pltpu.HBM)
    dma = pltpu.SemaphoreType.DMA
    y, _, _ = pl.pallas_call(
        sync_kernel,
        name="sync_kernel",
        out_shape=(
            jax.ShapeDtypeStruct((tokens, width), jnp.bfloat16),
            jax.ShapeDtypeStruct((chunks, 4, depth, COLS), jnp.bfloat16),
            jax.ShapeDtypeStruct((chunks, 4, COLS, depth), jnp.bfloat16),
        ),
        in_specs=[pl.BlockSpec(memory_space=pltpu.SMEM)] + [any_spec] * 7,
        out_specs=(any_spec,) * 3,
        scratch_shapes=[
            pltpu.VMEM((2, depth, COLS), jnp.float32),
            pltpu.VMEM((2, COLS, depth), jnp.float32),
            pltpu.VMEM((2, depth, COLS), jnp.float32),
            pltpu.VMEM((2, COLS, depth), jnp.float32),
            pltpu.VMEM((SENDS, depth, COLS), jnp.bfloat16),
            pltpu.VMEM((SENDS, COLS, depth), jnp.bfloat16),
            pltpu.VMEM((tokens, width), jnp.bfloat16),
            pltpu.VMEM((tokens, width), jnp.float32),
            pltpu.VMEM((2, width, COLS), jnp.bfloat16),
            pltpu.VMEM((2, COLS, width), jnp.bfloat16),
            pltpu.VMEM((2, 4, depth, COLS), jnp.bfloat16),
            pltpu.VMEM((2, 4, COLS, depth), jnp.bfloat16),
            pltpu.VMEM((width, COLS), jnp.bfloat16),
            pltpu.VMEM((COLS, width), jnp.bfloat16),
            pltpu.VMEM((tokens, COLS), jnp.bfloat16),
            dma((4, 2)), dma((2, SENDS)), dma((2, 2)), dma((2, 2)), dma((1,)),
        ] + [dma((2, chunks))] * 7,
        compiler_params=pltpu.CompilerParams(
            collective_id=0, has_side_effects=True, vmem_limit_bytes=62 * 1024 * 1024),
        cost_estimate=pl.CostEstimate(flops=4 * tokens * width * hid, bytes_accessed=8 * width * hid, transcendentals=0),
    )(lr, w_up, w_dn, g_up, g_dn, s_up, s_dn, x)
    return y


def solution(mesh):
    tp_width = mesh.shape["side"] // 2
    up_spec = P("side", None, "rep", None)
    down_spec = P("side", None, None, "rep")
    copy_spec = P("side", "rep", None, None, None)
    token_spec = P("side", "rep", None, None)

    def local_step(w_up, w_down, g_up, g_down, learn_rate, old_up, old_down, prompts):
        y = synced_output(learn_rate, w_up[0, 0], w_down[0, 0], g_up[0, 0], g_down[0, 0],
                          old_up[0, 0, 0], old_down[0, 0, 0], prompts[0, 0])
        is_gen = lax.axis_index("side") >= tp_width
        step_rate = learn_rate[0]
        new_up = w_up - step_rate * g_up
        new_down = w_down - step_rate * g_down
        y_local = jnp.where(is_gen, y, jnp.zeros_like(y))
        return new_up, new_down, y_local[None, None]

    return jax.shard_map(
        local_step,
        mesh=mesh,
        in_specs=(up_spec, down_spec, up_spec, down_spec, P(None), copy_spec, copy_spec, token_spec),
        out_specs=(up_spec, down_spec, token_spec),
        check_vma=False,
    )
```

```python
import functools

import jax
import jax.numpy as jnp
from jax import lax
from jax.experimental import pallas as pl
from jax.experimental.pallas import tpu as pltpu
from jax.sharding import PartitionSpec as P

MESH = pl.DeviceIdType.MESH
COLS = 256
SENDS = 4
TILE = 512


def gelu(x):
    return 0.5 * x * (1.0 + lax.erf(x * 0.7071067811865476))


def sync_kernel(lr, w_up, w_dn, g_up, g_dn, s_up, s_dn, x_hbm, y_hbm, land_up, land_dn, nw_up, nw_dn,
                wb_up, wb_dn, gb_up, gb_dn, d_up, d_dn, nb_up, nb_dn,
                x_v, acc, sb_up, sb_dn, lb_up, lb_dn, wg_up, wg_dn, u_v,
                t_sem, w_sem, send_sem, s_sem, l_sem, x_sem, out_sem,
                y_recv, x_recv, o_recv, n_recv, x_send, o_send, n_send):
    side, rep = lax.axis_index("side"), lax.axis_index("rep")
    other = 1 - side
    sib = rep + 1 - 2 * (rep % 2)
    cross = (rep + 2) % 4
    chunks = land_up.shape[0]
    depth = w_up.shape[0]
    lands, smalls = (land_up, land_dn), (d_up, d_dn)

    barrier = pltpu.get_barrier_semaphore()
    for dev in ((other, rep), (side, sib), (side, cross)):
        pl.semaphore_signal(barrier, inc=1, device_id=dev, device_id_type=MESH)

    def span(m):
        return pl.ds(pl.multiple_of(m * COLS, COLS), COLS)

    @pl.when(side == 0)
    def trainer():
        mats = ((w_up, g_up, wb_up, gb_up, nb_up, nw_up), (w_dn, g_dn, wb_dn, gb_dn, nb_dn, nw_dn))

        def part(h, ref, m):
            return ref.at[:, span(m)] if h == 0 else ref.at[span(m), :]

        def loads(h, m):
            w, g, wb, gb, _, _ = mats[h]
            k = m % 2
            return [
                pltpu.make_async_copy(part(h, w, m), wb.at[k], t_sem.at[2 * h, k]),
                pltpu.make_async_copy(part(h, g, m), gb.at[k], t_sem.at[2 * h + 1, k]),
            ]

        def store(h, m):
            return pltpu.make_async_copy(mats[h][4].at[m % 2], part(h, mats[h][5], m), w_sem.at[h, m % 2])

        def send(h, m):
            return pltpu.make_async_remote_copy(
                src_ref=smalls[h].at[m % SENDS], dst_ref=lands[h].at[m, rep],
                send_sem=send_sem.at[h, m % SENDS], recv_sem=y_recv.at[h, m],
                device_id=(other, rep), device_id_type=MESH)

        for m in range(2):
            for h in range(2):
                for c in loads(h, m):
                    c.start()
        rate = lr[0]

        def make(h, m):
            _, _, wb, gb, nb, _ = mats[h]
            k = m % 2
            for c in loads(h, m):
                c.wait()

            @pl.when(m >= SENDS)
            def _():
                send(h, m - SENDS).wait_send()

            @pl.when(m >= 2)
            def _():
                store(h, m - 2).wait()
            old = wb[k]
            new = old - rate * gb[k]
            nb[k] = new
            smalls[h][m % SENDS] = (new - old).astype(jnp.bfloat16)

            @pl.when(m + 2 < chunks)
            def _():
                for c in loads(h, m + 2):
                    c.start()

        make(0, 0)
        pl.semaphore_wait(barrier, 3)

        def step(m, _):
            @pl.when(m + 1 < chunks)
            def _():
                make(0, m + 1)

            @pl.when(m == 0)
            def _():
                send(0, 0).start()
                store(0, 0).start()

            @pl.when(m >= 1)
            def _():
                send(1, m - 1).start()
                store(1, m - 1).start()
            make(1, m)

            @pl.when(m + 1 < chunks)
            def _():
                send(0, m + 1).start()
                store(0, m + 1).start()
            return 0

        lax.fori_loop(0, chunks, step, 0)
        send(1, chunks - 1).start()
        store(1, chunks - 1).start()
        for h in range(2):
            for m in range(chunks - 2, chunks):
                store(h, m).wait()
        for m in range(chunks - SENDS, chunks):
            for h in range(2):
                send(h, m).wait_send()

    @pl.when(side == 1)
    def generator():
        def hop(h, m, row, dev, send, recv):
            return pltpu.make_async_remote_copy(
                src_ref=lands[h].at[m, row], dst_ref=lands[h].at[m, row],
                send_sem=send.at[h, m], recv_sem=recv.at[h, m],
                device_id=(side, dev), device_id_type=MESH)

        def from_trainer(h, m):
            return hop(h, m, rep, sib, x_send, y_recv)

        def across(h, m, row):
            return hop(h, m, row, cross, x_send, x_recv)

        def own(h, m, row):
            return hop(h, m, row, sib, o_send, o_recv)

        def next_own(h, m, row):
            return hop(h, m, row, sib, n_send, n_recv)

        sib_cross = (sib + 2) % 4
        stales = (sb_up, sb_dn)

        def stale(h, m):
            src = s_up.at[:, span(m)] if h == 0 else s_dn.at[span(m), :]
            return pltpu.make_async_copy(src, stales[h].at[m % 2], s_sem.at[h, m % 2])

        def landed(h, m):
            return pltpu.make_async_copy(lands[h].at[m], (lb_up, lb_dn)[h], l_sem.at[h])

        x_in = pltpu.make_async_copy(x_hbm, x_v, x_sem.at[0])
        x_in.start()
        for m in range(2):
            for h in range(2):
                stale(h, m).start()
        acc[...] = jnp.zeros_like(acc)
        x_in.wait()
        pl.semaphore_wait(barrier, 3)

        def pass_on(h, m):
            from_trainer(h, m).wait_recv()
            across(h, m, rep).start()
            own(h, m, rep).start()

        def turn(h, m):
            across(h, m, cross).wait_recv()
            next_own(h, m, cross).start()

        def fetch(h, m):
            own(h, m, sib).wait_recv()
            next_own(h, m, sib_cross).wait_recv()
            landed(h, m).start()

        tiles = x_v.shape[0] // TILE

        def up(m):
            k = m % 2
            stale(0, m).wait()
            landed(0, m).wait()
            for r in range(4):
                rows = pl.ds(r * depth, depth)
                wg_up[rows, :] = (sb_up[k, rows, :].astype(jnp.float32) + lb_up[r].astype(jnp.float32)).astype(jnp.bfloat16)

            @pl.when(m + 2 < chunks)
            def _():
                stale(0, m + 2).start()

            def tile(i, _):
                rows = pl.ds(pl.multiple_of(i * TILE, TILE), TILE)
                pre = jnp.dot(x_v[rows, :], wg_up[...], preferred_element_type=jnp.float32)
                u_v[k, rows, :] = gelu(pre).astype(jnp.bfloat16)
                return 0
            lax.fori_loop(0, tiles, tile, 0)

        def down_weights(m):
            k = m % 2
            stale(1, m).wait()
            landed(1, m).wait()
            for r in range(4):
                cols = pl.ds(r * depth, depth)
                wg_dn[:, cols] = (sb_dn[k, :, cols].astype(jnp.float32) + lb_dn[r].astype(jnp.float32)).astype(jnp.bfloat16)

        def down(m):
            down_weights(m)

            @pl.when(m + 2 < chunks)
            def _():
                stale(1, m + 2).start()

            def tile(i, _):
                rows = pl.ds(pl.multiple_of(i * TILE, TILE), TILE)
                acc[rows, :] += jnp.dot(u_v[m % 2, rows, :], wg_dn[...], preferred_element_type=jnp.float32)
                return 0
            lax.fori_loop(0, tiles, tile, 0)

        pass_on(0, 0)

        def step(m, _):
            pass_on(0, m)
            turn(0, m - 1)

            @pl.when(m >= 3)
            def _():
                down(m - 3)
            fetch(0, m - 1)
            pass_on(1, m - 1)

            @pl.when(m >= 2)
            def _():
                turn(1, m - 2)
            up(m - 1)

            @pl.when(m >= 2)
            def _():
                fetch(1, m - 2)
            return 0

        lax.fori_loop(1, chunks, step, 0)
        last = chunks - 1
        turn(0, last)
        down(last - 2)
        fetch(0, last)
        pass_on(1, last)
        up(last)
        turn(1, last - 1)
        fetch(1, last - 1)
        down(last - 1)
        turn(1, last)
        fetch(1, last)
        down_weights(last)

        def y_out(i):
            rows = pl.ds(pl.multiple_of(i * TILE, TILE), TILE)
            return pltpu.make_async_copy(x_v.at[rows, :], y_hbm.at[rows, :], out_sem.at[i])

        def tile(i, _):
            rows = pl.ds(pl.multiple_of(i * TILE, TILE), TILE)
            p = acc[rows, :] + jnp.dot(u_v[last % 2, rows, :], wg_dn[...], preferred_element_type=jnp.float32)
            x_v[rows, :] = (x_v[rows, :].astype(jnp.float32) + p).astype(jnp.bfloat16)

            @pl.when(i >= 1)
            def _():
                y_out(i - 1).start()
            return 0
        lax.fori_loop(0, tiles, tile, 0)

        def drain(m, _):
            for h in range(2):
                across(h, m, rep).wait_send()
                own(h, m, rep).wait_send()
                next_own(h, m, cross).wait_send()
            return 0
        lax.fori_loop(0, chunks, drain, 0)
        y_out(tiles - 1).start()
        for i in range(tiles):
            y_out(i).wait()


def finish_kernel(y_hbm, nw_up, nw_dn, new_up, new_dn, y_out, b_up, b_dn, b_y, in_sem, out_sem):
    side = lax.axis_index("side")
    n, rows, cols = b_up.shape
    ny = b_y.shape[0]
    row_y = b_y.shape[1]

    def piece(ref, h, i):
        return ref.at[:, pl.ds(i * cols, cols)] if h == 0 else ref.at[pl.ds(i * cols, cols), :]

    def y_piece(ref, i):
        return ref.at[pl.ds(i * row_y, row_y), :]

    mats = ((nw_up, b_up, new_up), (nw_dn, b_dn, new_dn))

    @pl.when(side == 0)
    def trainer():
        def read(h, i):
            return pltpu.make_async_copy(piece(mats[h][0], h, i), mats[h][1].at[i], in_sem.at[h, i])

        def write(h, i):
            return pltpu.make_async_copy(mats[h][1].at[i], piece(mats[h][2], h, i), out_sem.at[h, i])

        def write_y(i):
            return pltpu.make_async_copy(b_y.at[0], y_piece(y_out, i), out_sem.at[2, i])

        for i in range(n):
            for h in range(2):
                read(h, i).start()
        b_y[0] = jnp.zeros_like(b_y[0])
        for i in range(n):
            for h in range(2):
                read(h, i).wait()
                write(h, i).start()
        for i in range(ny):
            write_y(i).start()
        for i in range(n):
            for h in range(2):
                write(h, i).wait()
        for i in range(ny):
            write_y(i).wait()

    @pl.when(side == 1)
    def generator():
        def write(h, i):
            return pltpu.make_async_copy(mats[h][1].at[0], piece(mats[h][2], h, i), out_sem.at[h, i])

        def read_y(i):
            return pltpu.make_async_copy(y_piece(y_hbm, i), b_y.at[i], in_sem.at[2, i])

        def write_y(i):
            return pltpu.make_async_copy(b_y.at[i], y_piece(y_out, i), out_sem.at[2, i])

        for i in range(ny):
            read_y(i).start()
        b_up[0] = jnp.zeros_like(b_up[0])
        b_dn[0] = jnp.zeros_like(b_dn[0])
        for i in range(ny):
            read_y(i).wait()
            write_y(i).start()
        for i in range(n):
            for h in range(2):
                write(h, i).start()
        for i in range(n):
            for h in range(2):
                write(h, i).wait()
        for i in range(ny):
            write_y(i).wait()


def step_outputs(lr, w_up, w_dn, g_up, g_dn, s_up, s_dn, x):
    depth, hid = w_up.shape
    tokens, width = x.shape
    chunks = hid // COLS
    any_spec = pl.BlockSpec(memory_space=pltpu.HBM)
    dma = pltpu.SemaphoreType.DMA
    vmem = pltpu.VMEM
    f32, bf16 = jnp.float32, jnp.bfloat16
    y, _, _, nw_up, nw_dn = pl.pallas_call(
        sync_kernel,
        name="sync_kernel",
        out_shape=(
            jax.ShapeDtypeStruct((tokens, width), bf16),
            jax.ShapeDtypeStruct((chunks, 4, depth, COLS), bf16),
            jax.ShapeDtypeStruct((chunks, 4, COLS, depth), bf16),
            jax.ShapeDtypeStruct(w_up.shape, f32),
            jax.ShapeDtypeStruct(w_dn.shape, f32),
        ),
        in_specs=[pl.BlockSpec(memory_space=pltpu.SMEM)] + [any_spec] * 7,
        out_specs=(any_spec,) * 5,
        scratch_shapes=[
            vmem((2, depth, COLS), f32), vmem((2, COLS, depth), f32),
            vmem((2, depth, COLS), f32), vmem((2, COLS, depth), f32),
            vmem((SENDS, depth, COLS), bf16), vmem((SENDS, COLS, depth), bf16),
            vmem((2, depth, COLS), f32), vmem((2, COLS, depth), f32),
            vmem((tokens, width), bf16), vmem((tokens, width), f32),
            vmem((2, width, COLS), bf16), vmem((2, COLS, width), bf16),
            vmem((4, depth, COLS), bf16), vmem((4, COLS, depth), bf16),
            vmem((width, COLS), bf16), vmem((COLS, width), bf16),
            vmem((2, tokens, COLS), bf16),
            dma((4, 2)), dma((2, 2)), dma((2, SENDS)), dma((2, 2)), dma((2,)), dma((1,)), dma((tokens // TILE,)),
        ] + [dma((2, chunks))] * 7,
        compiler_params=pltpu.CompilerParams(
            collective_id=0, has_side_effects=True, vmem_limit_bytes=60 * 1024 * 1024),
        cost_estimate=pl.CostEstimate(flops=4 * tokens * width * hid, bytes_accessed=8 * width * hid, transcendentals=0),
    )(lr, w_up, w_dn, g_up, g_dn, s_up, s_dn, x)
    piece = 1024
    return pl.pallas_call(
        finish_kernel,
        name="finish_kernel",
        out_shape=(
            jax.ShapeDtypeStruct(w_up.shape, f32),
            jax.ShapeDtypeStruct(w_dn.shape, f32),
            jax.ShapeDtypeStruct((tokens, width), bf16),
        ),
        in_specs=[any_spec] * 3,
        out_specs=(any_spec,) * 3,
        scratch_shapes=[
            vmem((hid // piece, depth, piece), f32), vmem((hid // piece, piece, depth), f32),
            vmem((4, tokens // 4, width), bf16),
            dma((3, hid // piece)), dma((3, hid // piece)),
        ],
        compiler_params=pltpu.CompilerParams(vmem_limit_bytes=60 * 1024 * 1024),
        cost_estimate=pl.CostEstimate(flops=0, bytes_accessed=20 * depth * hid, transcendentals=0),
    )(y, nw_up, nw_dn)


def solution(mesh):
    up_spec = P("side", None, "rep", None)
    down_spec = P("side", None, None, "rep")
    copy_spec = P("side", "rep", None, None, None)
    token_spec = P("side", "rep", None, None)

    def local_step(w_up, w_down, g_up, g_down, learn_rate, old_up, old_down, prompts):
        new_up, new_down, y = step_outputs(
            learn_rate, w_up[0, 0], w_down[0, 0], g_up[0, 0], g_down[0, 0],
            old_up[0, 0, 0], old_down[0, 0, 0], prompts[0, 0])
        return new_up[None, None], new_down[None, None], y[None, None]

    return jax.shard_map(
        local_step,
        mesh=mesh,
        in_specs=(up_spec, down_spec, up_spec, down_spec, P(None), copy_spec, copy_spec, token_spec),
        out_specs=(up_spec, down_spec, token_spec),
        check_vma=False,
    )
```

```python
import functools

import jax
import jax.numpy as jnp
from jax import lax
from jax.experimental import pallas as pl
from jax.experimental.pallas import tpu as pltpu
from jax.sharding import PartitionSpec as P

MESH = pl.DeviceIdType.MESH
COLS = 256
SENDS = 4
TILE = 1024
HALF = COLS // 2
VMEM_SYNC = 16 * 1024 * 1024
VMEM_FINISH = 16 * 1024 * 1024


def gelu(x):
    return 0.5 * x * (1.0 + lax.erf(x * 0.7071067811865476))


def sync_kernel(lr, w_up, w_dn, g_up, g_dn, s_up, s_dn, x_hbm,
                land_up, land_dn, x_v, acc, new_dn, u_v, sb_dn, last_dn,
                wb_up, wb_dn, gb_up, gb_dn, d_up, d_dn, sb_up, lb_up, lb_dn, wg_up, wg_dn,
                t_sem, send_sem, s_sem, l_sem, x_sem,
                y_recv, x_recv, o_recv, n_recv, x_send, o_send, n_send,
                yt_recv, xt_recv, ot_recv, nt_recv, xt_send, ot_send, nt_send):
    side, rep = lax.axis_index("side"), lax.axis_index("rep")
    other = 1 - side
    sib = rep + 1 - 2 * (rep % 2)
    cross = (rep + 2) % 4
    sib_cross = (sib + 2) % 4
    chunks = land_up.shape[0]
    depth = w_up.shape[0]
    tokens, width = x_v.shape
    lands, smalls = (land_up, land_dn), (d_up, d_dn)
    last = chunks - 1

    barrier = pltpu.get_barrier_semaphore()
    for dev in ((other, rep), (side, sib), (side, cross)):
        pl.semaphore_signal(barrier, inc=1, device_id=dev, device_id_type=MESH)

    def span(m):
        return pl.ds(pl.multiple_of(m * COLS, COLS), COLS)

    def late(row, q):
        return last_dn.at[row, pl.ds(q * HALF, HALF), :]

    @pl.when(side == 0)
    def trainer():
        mats = ((w_up, g_up, wb_up, gb_up), (w_dn, g_dn, wb_dn, gb_dn))

        def part(h, ref, m):
            return ref.at[:, span(m)] if h == 0 else ref.at[span(m), :]

        def loads(h, m):
            w, g, wb, gb = mats[h]
            k = m % 2
            return [
                pltpu.make_async_copy(part(h, w, m), wb.at[k], t_sem.at[2 * h, k]),
                pltpu.make_async_copy(part(h, g, m), gb.at[k], t_sem.at[2 * h + 1, k]),
            ]

        def send(h, m):
            return pltpu.make_async_remote_copy(
                src_ref=smalls[h].at[m % SENDS], dst_ref=lands[h].at[m, rep],
                send_sem=send_sem.at[h, m % SENDS], recv_sem=y_recv.at[h, m],
                device_id=(other, rep), device_id_type=MESH)

        def send_late(q):
            m = last - 1 + q // 2
            return pltpu.make_async_remote_copy(
                src_ref=d_dn.at[m % SENDS, pl.ds((q % 2) * HALF, HALF), :], dst_ref=late(rep, q),
                send_sem=xt_send.at[q], recv_sem=yt_recv.at[q],
                device_id=(other, rep), device_id_type=MESH)

        for m in range(2):
            for h in range(2):
                for c in loads(h, m):
                    c.start()
        rate = lr[0]

        def make(h, m):
            k = m % 2
            for c in loads(h, m):
                c.wait()

            @pl.when(m >= SENDS)
            def _():
                send(h, m - SENDS).wait_send()
            old = mats[h][2][k]
            new = old - rate * mats[h][3][k]
            if h == 0:
                acc[:, span(m)] = new
            else:
                new_dn[span(m), :] = new
            smalls[h][m % SENDS] = (new - old).astype(jnp.bfloat16)

            @pl.when(m + 2 < chunks)
            def _():
                for c in loads(h, m + 2):
                    c.start()

        make(0, 0)
        pl.semaphore_wait(barrier, 3)

        def step(m, _):
            make(0, m + 1)

            @pl.when(m == 0)
            def _():
                send(0, 0).start()

            @pl.when(m >= 1)
            def _():
                send(1, m - 1).start()
            make(1, m)
            send(0, m + 1).start()
            return 0

        lax.fori_loop(0, last, step, 0)
        make(1, last)
        for q in range(4):
            send_late(q).start()
        for m in range(chunks - SENDS, chunks):
            send(0, m).wait_send()
        for m in range(chunks - SENDS, last - 1):
            send(1, m).wait_send()
        for q in range(4):
            send_late(q).wait_send()

    @pl.when(side == 1)
    def generator():
        def hop(h, m, row, dev, send, recv):
            return pltpu.make_async_remote_copy(
                src_ref=lands[h].at[m, row], dst_ref=lands[h].at[m, row],
                send_sem=send.at[h, m], recv_sem=recv.at[h, m],
                device_id=(side, dev), device_id_type=MESH)

        def from_trainer(h, m):
            return hop(h, m, rep, sib, x_send, y_recv)

        def across(h, m, row):
            return hop(h, m, row, cross, x_send, x_recv)

        def own(h, m, row):
            return hop(h, m, row, sib, o_send, o_recv)

        def next_own(h, m, row):
            return hop(h, m, row, sib, n_send, n_recv)

        def late_hop(q, row, dev, send, recv):
            return pltpu.make_async_remote_copy(
                src_ref=late(row, q), dst_ref=late(row, q), send_sem=send.at[q], recv_sem=recv.at[q],
                device_id=(side, dev), device_id_type=MESH)

        stales = (sb_up, sb_dn)

        def stale(h, m):
            src = s_up.at[:, span(m)] if h == 0 else s_dn.at[span(m), :]
            return pltpu.make_async_copy(src, stales[h].at[m % 2], s_sem.at[h, m % 2])

        def landed(h, m):
            return pltpu.make_async_copy(lands[h].at[m], (lb_up, lb_dn)[h], l_sem.at[h])

        x_in = pltpu.make_async_copy(x_hbm, x_v, x_sem.at[0])
        x_in.start()
        for m in range(2):
            for h in range(2):
                stale(h, m).start()
        pl.semaphore_wait(barrier, 3)

        def pass_on(h, m):
            from_trainer(h, m).wait_recv()
            across(h, m, rep).start()
            own(h, m, rep).start()

        def pass_late(q):
            late_hop(q, rep, sib, xt_send, yt_recv).wait_recv()
            late_hop(q, rep, cross, xt_send, xt_recv).start()
            late_hop(q, rep, sib, ot_send, ot_recv).start()

        def turn(h, m):
            across(h, m, cross).wait_recv()
            next_own(h, m, cross).start()

        def turn_late(q):
            late_hop(q, cross, cross, xt_send, xt_recv).wait_recv()
            late_hop(q, cross, sib, nt_send, nt_recv).start()

        def fetch(h, m):
            own(h, m, sib).wait_recv()
            next_own(h, m, sib_cross).wait_recv()
            landed(h, m).start()

        tiles = tokens // TILE
        groups = TILE // depth

        def tile_rows(i):
            return pl.ds(pl.multiple_of(i * TILE, TILE), TILE)

        def u_cols(m):
            return pl.ds(pl.multiple_of((m % 2) * COLS, COLS), COLS)

        def up(m):
            k = m % 2
            stale(0, m).wait()
            landed(0, m).wait()
            for r in range(4):
                rows = pl.ds(r * depth, depth)
                wg_up[rows, :] = (sb_up[k, rows, :].astype(jnp.float32) + lb_up[r].astype(jnp.float32)).astype(jnp.bfloat16)

            @pl.when(m + 2 < chunks)
            def _():
                stale(0, m + 2).start()

            def tile(i, _):
                pre = jnp.dot(x_v[tile_rows(i), :], wg_up[...], preferred_element_type=jnp.float32)
                u_v[tile_rows(i), u_cols(m)] = gelu(pre).astype(jnp.bfloat16)
                return 0
            lax.fori_loop(0, tiles, tile, 0)

        def down(m):
            k = m % 2
            stale(1, m).wait()
            landed(1, m).wait()
            for r in range(4):
                cols = pl.ds(r * depth, depth)
                wg_dn[:, cols] = (sb_dn[k, :, cols].astype(jnp.float32) + lb_dn[r].astype(jnp.float32)).astype(jnp.bfloat16)

            @pl.when(m + 2 < chunks)
            def _():
                stale(1, m + 2).start()

            def tile(i, _):
                p = jnp.dot(u_v[tile_rows(i), u_cols(m)], wg_dn[...], preferred_element_type=jnp.float32)
                for g in range(groups):
                    cols = pl.ds(pl.multiple_of((i * groups + g) * width, width), width)
                    acc[:, cols] += p[g * depth:(g + 1) * depth]
                return 0
            lax.fori_loop(0, tiles, tile, 0)

        pass_on(0, 0)
        x_in.wait()

        def clear(i, _):
            cols = pl.ds(pl.multiple_of(i * width, width), width)
            rows = pl.ds(pl.multiple_of(i * depth, depth), depth)
            acc[:, cols] = x_v[rows, :].astype(jnp.float32)
            return 0
        lax.fori_loop(0, tokens // depth, clear, 0)

        def step(m, _):
            pass_on(0, m)
            turn(0, m - 1)

            @pl.when(m >= 3)
            def _():
                down(m - 3)
            fetch(0, m - 1)
            pass_on(1, m - 1)

            @pl.when(m >= 2)
            def _():
                turn(1, m - 2)
            up(m - 1)

            @pl.when(m >= 2)
            def _():
                fetch(1, m - 2)
            return 0

        lax.fori_loop(1, last, step, 0)
        pass_on(0, last)
        turn(0, last - 1)
        down(last - 3)
        fetch(0, last - 1)
        pass_late(0)
        turn(1, last - 2)
        up(last - 1)
        pass_late(1)
        fetch(1, last - 2)
        turn(0, last)
        pass_late(2)
        down(last - 2)
        fetch(0, last)
        pass_late(3)
        turn_late(0)
        up(last)
        for q in range(1, 4):
            turn_late(q)
        for m in range(last - 1, chunks):
            stale(1, m).wait()

        def drain(m, _):
            across(0, m, rep).wait_send()
            own(0, m, rep).wait_send()
            next_own(0, m, cross).wait_send()

            @pl.when(m < last - 1)
            def _():
                across(1, m, rep).wait_send()
                own(1, m, rep).wait_send()
                next_own(1, m, cross).wait_send()
            return 0
        lax.fori_loop(0, chunks, drain, 0)
        for q in range(4):
            late_hop(q, sib, sib, ot_send, ot_recv).wait_recv()
            late_hop(q, sib_cross, sib, nt_send, nt_recv).wait_recv()
        for q in range(4):
            late_hop(q, rep, cross, xt_send, xt_recv).wait_send()
            late_hop(q, rep, sib, ot_send, ot_recv).wait_send()
            late_hop(q, cross, sib, nt_send, nt_recv).wait_send()


def finish_kernel(x_v, acc, new_dn, u_v, sb_dn, last_dn, up_out, dn_out, y_out, wg, y_v, zero, sem, y_sem):
    side = lax.axis_index("side")
    depth = acc.shape[0]
    tokens, width = x_v.shape
    n = up_out.shape[1] // width
    rows_dn = dn_out.shape[0] // n
    blocks = tokens // depth
    pieces = width // zero.shape[1]

    def up_piece(i):
        return pl.ds(i * width, width)

    def dn_piece(i):
        return pl.ds(i * rows_dn, rows_dn)

    def y_piece(i):
        return y_out.at[pl.ds(i * depth, depth), :]

    @pl.when(side == 0)
    def trainer():
        copies = []
        for i in range(n):
            copies.append(pltpu.make_async_copy(acc.at[:, up_piece(i)], up_out.at[:, up_piece(i)], sem.at[0, i, 0]))
            copies.append(pltpu.make_async_copy(new_dn.at[dn_piece(i), :], dn_out.at[dn_piece(i), :], sem.at[1, i, 0]))
        for c in copies:
            c.start()
        y_v[0] = jnp.zeros_like(y_v[0])
        ys = [pltpu.make_async_copy(y_v.at[0], y_piece(i), y_sem.at[i]) for i in range(blocks)]
        for c in ys:
            c.start()
        for c in copies + ys:
            c.wait()

    @pl.when(side == 1)
    def generator():
        zero[...] = jnp.zeros_like(zero)
        size = zero.shape[1]
        copies = []
        for i in range(n):
            for j in range(pieces):
                copies.append(pltpu.make_async_copy(
                    zero, up_out.at[:, pl.ds(i * width + j * size, size)], sem.at[0, i, j]))
                copies.append(pltpu.make_async_copy(
                    zero, dn_out.at[pl.ds(i * rows_dn + j * depth, depth), :], sem.at[1, i, j]))
        for k in range(2):
            ks = pl.ds(k * COLS, COLS)
            for r in range(4):
                cols = pl.ds(r * depth, depth)
                wg[ks, cols] = (sb_dn[k, :, cols].astype(jnp.float32) + last_dn[r, ks, :].astype(jnp.float32)).astype(jnp.bfloat16)
        for c in copies:
            c.start()

        def out(i):
            return pltpu.make_async_copy(y_v.at[i], y_out.at[pl.ds(pl.multiple_of(i * depth, depth), depth), :], y_sem.at[i])

        def block(i, _):
            rows = pl.ds(pl.multiple_of(i * depth, depth), depth)
            cols = pl.ds(pl.multiple_of(i * width, width), width)
            p = jnp.dot(u_v[rows, :], wg[...], preferred_element_type=jnp.float32)
            y_v[i] = (acc[:, cols] + p).astype(jnp.bfloat16)

            @pl.when(i >= 1)
            def _():
                out(i - 1).start()
            return 0
        lax.fori_loop(0, blocks, block, 0)
        for c in copies:
            c.wait()
        out(blocks - 1).start()
        for i in range(blocks):
            out(i).wait()


def step_outputs(lr, w_up, w_dn, g_up, g_dn, s_up, s_dn, x):
    depth, hid = w_up.shape
    tokens, width = x.shape
    chunks = hid // COLS
    any_spec = pl.BlockSpec(memory_space=pltpu.HBM)
    vmem_spec = pl.BlockSpec(memory_space=pltpu.VMEM)
    dma = pltpu.SemaphoreType.DMA
    vmem = pltpu.VMEM
    f32, bf16 = jnp.float32, jnp.bfloat16
    _, _, *held = pl.pallas_call(
        sync_kernel,
        name="sync_kernel",
        out_shape=(
            jax.ShapeDtypeStruct((chunks, 4, depth, COLS), bf16),
            jax.ShapeDtypeStruct((chunks, 4, COLS, depth), bf16),
            vmem((tokens, width), bf16),
            vmem(w_up.shape, f32),
            vmem(w_dn.shape, f32),
            vmem((tokens, 2 * COLS), bf16),
            vmem((2, COLS, width), bf16),
            vmem((4, 2 * COLS, depth), bf16),
        ),
        in_specs=[pl.BlockSpec(memory_space=pltpu.SMEM)] + [any_spec] * 7,
        out_specs=(any_spec,) * 2 + (vmem_spec,) * 6,
        scratch_shapes=[
            vmem((2, depth, COLS), f32), vmem((2, COLS, depth), f32),
            vmem((2, depth, COLS), f32), vmem((2, COLS, depth), f32),
            vmem((SENDS, depth, COLS), bf16), vmem((SENDS, COLS, depth), bf16),
            vmem((2, width, COLS), bf16),
            vmem((4, depth, COLS), bf16), vmem((4, COLS, depth), bf16),
            vmem((width, COLS), bf16), vmem((COLS, width), bf16),
            dma((4, 2)), dma((2, SENDS)), dma((2, 2)), dma((2,)), dma((1,)),
        ] + [dma((2, chunks))] * 7 + [dma((4,))] * 7,
        compiler_params=pltpu.CompilerParams(
            collective_id=0, has_side_effects=True, vmem_limit_bytes=VMEM_SYNC),
        cost_estimate=pl.CostEstimate(flops=4 * tokens * width * hid, bytes_accessed=8 * width * hid, transcendentals=0),
    )(lr, w_up, w_dn, g_up, g_dn, s_up, s_dn, x)
    n = hid // width
    return pl.pallas_call(
        finish_kernel,
        name="finish_kernel",
        out_shape=(
            jax.ShapeDtypeStruct(w_up.shape, f32),
            jax.ShapeDtypeStruct(w_dn.shape, f32),
            jax.ShapeDtypeStruct((tokens, width), bf16),
        ),
        in_specs=[vmem_spec] * 6,
        out_specs=(any_spec,) * 3,
        scratch_shapes=[
            vmem((2 * COLS, width), bf16), vmem((tokens // depth, depth, width), bf16), vmem((depth, depth), f32),
            dma((2, n, width // depth)), dma((tokens // depth,)),
        ],
        compiler_params=pltpu.CompilerParams(vmem_limit_bytes=VMEM_FINISH),
        cost_estimate=pl.CostEstimate(flops=4 * tokens * width * COLS, bytes_accessed=12 * depth * hid, transcendentals=0),
    )(*[pltpu.with_memory_space_constraint(a, pltpu.VMEM) for a in held])


def solution(mesh):
    up_spec = P("side", None, "rep", None)
    down_spec = P("side", None, None, "rep")
    copy_spec = P("side", "rep", None, None, None)
    token_spec = P("side", "rep", None, None)

    def local_step(w_up, w_down, g_up, g_down, learn_rate, old_up, old_down, prompts):
        new_up, new_down, y = step_outputs(
            learn_rate, w_up[0, 0], w_down[0, 0], g_up[0, 0], g_down[0, 0],
            old_up[0, 0, 0], old_down[0, 0, 0], prompts[0, 0])
        return new_up[None, None], new_down[None, None], y[None, None]

    return jax.shard_map(
        local_step,
        mesh=mesh,
        in_specs=(up_spec, down_spec, up_spec, down_spec, P(None), copy_spec, copy_spec, token_spec),
        out_specs=(up_spec, down_spec, token_spec),
        check_vma=False,
    )
```

```python
import functools

import jax
import jax.numpy as jnp
from jax import lax
from jax.experimental import pallas as pl
from jax.experimental.pallas import tpu as pltpu
from jax.sharding import PartitionSpec as P

MESH = pl.DeviceIdType.MESH
COLS = 256
SENDS = 4
TILE = 1024
HALF = COLS // 2
VMEM_SYNC = 14 * 1024 * 1024
VMEM_FINISH = 14 * 1024 * 1024


def gelu(x):
    return 0.5 * x * (1.0 + lax.erf(x * 0.7071067811865476))


def sync_kernel(lr_hbm, w_up, w_dn, g_up, g_dn, s_up, s_dn, x_hbm,
                land_up, land_dn, x_v, acc, new_dn, u_v, sb_up, sb_dn, last_dn, zero,
                wb_up, wb_dn, gb_up, gb_dn, d_up, d_dn, swap_dn, lb_up, lb_dn, wg_up, wg_dn,
                lr, t_sem, send_sem, s_sem, l_sem, x_sem,
                y_recv, x_recv, o_recv, n_recv, x_send, o_send, n_send,
                yt_recv, xt_recv, ot_recv, nt_recv, xt_send, ot_send, nt_send, swap_sem):
    side, rep = lax.axis_index("side"), lax.axis_index("rep")
    other = 1 - side
    sib = rep + 1 - 2 * (rep % 2)
    cross = (rep + 2) % 4
    sib_cross = (sib + 2) % 4
    chunks = land_up.shape[0]
    depth = w_up.shape[0]
    tokens, width = x_v.shape
    lands, smalls = (land_up, land_dn), (d_up, d_dn)
    last = chunks - 1

    barrier = pltpu.get_barrier_semaphore()
    for dev in ((other, rep), (side, sib), (side, cross)):
        pl.semaphore_signal(barrier, inc=1, device_id=dev, device_id_type=MESH)

    def span(m):
        return pl.ds(pl.multiple_of(m * COLS, COLS), COLS)

    def late(row, q):
        return last_dn.at[row, pl.ds(q * HALF, HALF), :]

    @pl.when(side == 0)
    def trainer():
        mats = ((w_up, g_up, wb_up, gb_up), (w_dn, g_dn, wb_dn, gb_dn))

        def part(h, ref, m):
            return ref.at[:, span(m)] if h == 0 else ref.at[span(m), :]

        def loads(h, m):
            w, g, wb, gb = mats[h]
            k = m % 2
            return [
                pltpu.make_async_copy(part(h, w, m), wb.at[k], t_sem.at[2 * h, k]),
                pltpu.make_async_copy(part(h, g, m), gb.at[k], t_sem.at[2 * h + 1, k]),
            ]

        def send(h, m):
            return pltpu.make_async_remote_copy(
                src_ref=smalls[h].at[m % SENDS], dst_ref=lands[h].at[m, rep],
                send_sem=send_sem.at[h, m % SENDS], recv_sem=y_recv.at[h, m],
                device_id=(other, rep), device_id_type=MESH)

        def send_late(q):
            m = last - 1 + q // 2
            return pltpu.make_async_remote_copy(
                src_ref=d_dn.at[m % SENDS, pl.ds((q % 2) * HALF, HALF), :], dst_ref=late(rep, q),
                send_sem=xt_send.at[q], recv_sem=yt_recv.at[q],
                device_id=(other, rep), device_id_type=MESH)

        swap = pltpu.make_async_remote_copy(
            src_ref=d_dn.at[last % SENDS, pl.ds(HALF, HALF), :], dst_ref=swap_dn,
            send_sem=swap_sem.at[0], recv_sem=swap_sem.at[1],
            device_id=(side, cross), device_id_type=MESH)
        send_swapped = pltpu.make_async_remote_copy(
            src_ref=swap_dn, dst_ref=late(cross, 3),
            send_sem=xt_send.at[4], recv_sem=yt_recv.at[4],
            device_id=(other, rep), device_id_type=MESH)

        lr_in = pltpu.make_async_copy(lr_hbm, lr, x_sem.at[0])
        lr_in.start()
        for c in loads(0, 0):
            c.start()
        lr_in.wait()
        rate = lr[0]

        def make(h, m):
            k = m % 2
            for c in loads(h, m):
                c.wait()

            @pl.when(m >= SENDS)
            def _():
                send(h, m - SENDS).wait_send()
            old = mats[h][2][k]
            new = old - rate * mats[h][3][k]
            if h == 0:
                acc[:, span(m)] = new
            else:
                new_dn[span(m), :] = new
            smalls[h][m % SENDS] = (new - old).astype(jnp.bfloat16)

            @pl.when(m + 2 < chunks)
            def _():
                for c in loads(h, m + 2):
                    c.start()

        make(0, 0)
        for h, m in ((0, 1), (1, 0), (1, 1)):
            for c in loads(h, m):
                c.start()
        pl.semaphore_wait(barrier, 3)
        send(0, 0).start()

        def step(m, _):
            make(0, m + 1)

            @pl.when(m >= 1)
            def _():
                send(1, m - 1).start()
            make(1, m)
            send(0, m + 1).start()
            return 0

        lax.fori_loop(0, last, step, 0)
        make(1, last)
        for q in range(4):
            send_late(q).start()
        swap.start()
        swap.wait_recv()
        send_swapped.start()
        swap.wait_send()
        for m in range(chunks - SENDS, chunks):
            send(0, m).wait_send()
        for m in range(chunks - SENDS, last - 1):
            send(1, m).wait_send()
        for q in range(4):
            send_late(q).wait_send()
        send_swapped.wait_send()

    @pl.when(side == 1)
    def generator():
        def hop(h, m, row, dev, send, recv):
            return pltpu.make_async_remote_copy(
                src_ref=lands[h].at[m, row], dst_ref=lands[h].at[m, row],
                send_sem=send.at[h, m], recv_sem=recv.at[h, m],
                device_id=(side, dev), device_id_type=MESH)

        def from_trainer(h, m):
            return hop(h, m, rep, sib, x_send, y_recv)

        def across(h, m, row):
            return hop(h, m, row, cross, x_send, x_recv)

        def own(h, m, row):
            return hop(h, m, row, sib, o_send, o_recv)

        def next_own(h, m, row):
            return hop(h, m, row, sib, n_send, n_recv)

        def late_hop(q, row, dev, send, recv):
            return pltpu.make_async_remote_copy(
                src_ref=late(row, q), dst_ref=late(row, q), send_sem=send.at[q], recv_sem=recv.at[q],
                device_id=(side, dev), device_id_type=MESH)

        stales = (sb_up, sb_dn)

        def stale(h, m):
            src = s_up.at[:, span(m)] if h == 0 else s_dn.at[span(m), :]
            return pltpu.make_async_copy(src, stales[h].at[m % 2], s_sem.at[h, m % 2])

        def landed(h, m):
            return pltpu.make_async_copy(lands[h].at[m], (lb_up, lb_dn)[h], l_sem.at[h])

        x_in = pltpu.make_async_copy(x_hbm, x_v, x_sem.at[0])
        x_in.start()
        for m in range(2):
            for h in range(2):
                stale(h, m).start()
        pl.semaphore_wait(barrier, 3)

        def pass_on(h, m):
            from_trainer(h, m).wait_recv()
            across(h, m, rep).start()
            own(h, m, rep).start()

        def pass_late(q):
            late_hop(q, rep, sib, xt_send, yt_recv).wait_recv()
            if q < 3:
                late_hop(q, rep, cross, xt_send, xt_recv).start()
            late_hop(q, rep, sib, ot_send, ot_recv).start()

        def turn(h, m):
            across(h, m, cross).wait_recv()
            next_own(h, m, cross).start()

        def turn_late(q):
            if q < 3:
                late_hop(q, cross, cross, xt_send, xt_recv).wait_recv()
            else:
                pltpu.make_async_remote_copy(
                    src_ref=late(cross, q), dst_ref=late(cross, q), send_sem=xt_send.at[4], recv_sem=yt_recv.at[4],
                    device_id=(side, sib), device_id_type=MESH).wait_recv()
            late_hop(q, cross, sib, nt_send, nt_recv).start()

        def fetch(h, m):
            own(h, m, sib).wait_recv()
            next_own(h, m, sib_cross).wait_recv()
            landed(h, m).start()

        tiles = tokens // TILE
        groups = TILE // depth

        def tile_rows(i):
            return pl.ds(pl.multiple_of(i * TILE, TILE), TILE)

        def u_cols(m):
            return pl.ds(pl.multiple_of((m % 2) * COLS, COLS), COLS)

        def up(m):
            k = m % 2
            stale(0, m).wait()
            landed(0, m).wait()
            for r in range(4):
                rows = pl.ds(r * depth, depth)
                wg_up[rows, :] = (sb_up[k, rows, :].astype(jnp.float32) + lb_up[r].astype(jnp.float32)).astype(jnp.bfloat16)

            @pl.when(m + 2 < chunks)
            def _():
                stale(0, m + 2).start()

            def tile(i, _):
                pre = jnp.dot(x_v[tile_rows(i), :], wg_up[...], preferred_element_type=jnp.float32)
                u_v[tile_rows(i), u_cols(m)] = gelu(pre).astype(jnp.bfloat16)
                return 0
            lax.fori_loop(0, tiles, tile, 0)

        def down(m):
            k = m % 2
            stale(1, m).wait()
            landed(1, m).wait()
            for r in range(4):
                cols = pl.ds(r * depth, depth)
                wg_dn[:, cols] = (sb_dn[k, :, cols].astype(jnp.float32) + lb_dn[r].astype(jnp.float32)).astype(jnp.bfloat16)

            @pl.when(m + 2 < chunks)
            def _():
                stale(1, m + 2).start()

            def tile(i, _):
                p = jnp.dot(u_v[tile_rows(i), u_cols(m)], wg_dn[...], preferred_element_type=jnp.float32)
                for g in range(groups):
                    cols = pl.ds(pl.multiple_of((i * groups + g) * width, width), width)
                    acc[:, cols] += p[g * depth:(g + 1) * depth]
                return 0
            lax.fori_loop(0, tiles, tile, 0)

        pass_on(0, 0)
        x_in.wait()
        zero[...] = jnp.zeros_like(zero)

        def clear(i, _):
            cols = pl.ds(pl.multiple_of(i * width, width), width)
            rows = pl.ds(pl.multiple_of(i * depth, depth), depth)
            acc[:, cols] = x_v[rows, :].astype(jnp.float32)
            return 0
        lax.fori_loop(0, tokens // depth, clear, 0)

        def step(m, _):
            pass_on(0, m)
            turn(0, m - 1)

            @pl.when(m >= 3)
            def _():
                down(m - 3)
            fetch(0, m - 1)
            pass_on(1, m - 1)

            @pl.when(m >= 2)
            def _():
                turn(1, m - 2)
            up(m - 1)

            @pl.when(m >= 2)
            def _():
                fetch(1, m - 2)
            return 0

        lax.fori_loop(1, last, step, 0)
        pass_on(0, last)
        turn(0, last - 1)
        down(last - 3)
        fetch(0, last - 1)
        pass_late(0)
        turn(1, last - 2)
        up(last - 1)
        pass_late(1)
        fetch(1, last - 2)
        turn(0, last)
        pass_late(2)
        down(last - 2)
        pass_late(3)
        for q in range(4):
            turn_late(q)
        stale(0, last).wait()
        for m in range(last - 1, chunks):
            stale(1, m).wait()
        own(0, last, sib).wait_recv()
        next_own(0, last, sib_cross).wait_recv()

        def drain(m, _):
            across(0, m, rep).wait_send()
            own(0, m, rep).wait_send()
            next_own(0, m, cross).wait_send()

            @pl.when(m < last - 1)
            def _():
                across(1, m, rep).wait_send()
                own(1, m, rep).wait_send()
                next_own(1, m, cross).wait_send()
            return 0
        lax.fori_loop(0, chunks, drain, 0)
        for q in range(4):
            late_hop(q, sib, sib, ot_send, ot_recv).wait_recv()
            late_hop(q, sib_cross, sib, nt_send, nt_recv).wait_recv()
        for q in range(4):
            if q < 3:
                late_hop(q, rep, cross, xt_send, xt_recv).wait_send()
            late_hop(q, rep, sib, ot_send, ot_recv).wait_send()
            late_hop(q, cross, sib, nt_send, nt_recv).wait_send()


def finish_kernel(x_v, acc, new_dn, u_v, sb_up, sb_dn, last_dn, zero, land_up, up_out, dn_out, y_out,
                  wg_up, wg, y_v, u_last, lb_up, sem, y_sem, l_sem):
    side = lax.axis_index("side")
    depth = acc.shape[0]
    tokens, width = x_v.shape
    n = up_out.shape[1] // width
    rows_dn = dn_out.shape[0] // n
    blocks = tokens // depth
    pieces = width // zero.shape[1]

    def up_piece(i):
        return pl.ds(i * width, width)

    def dn_piece(i):
        return pl.ds(i * rows_dn, rows_dn)

    def y_piece(i):
        return y_out.at[pl.ds(i * depth, depth), :]

    @pl.when(side == 0)
    def trainer():
        copies = []
        for i in range(n):
            copies.append(pltpu.make_async_copy(acc.at[:, up_piece(i)], up_out.at[:, up_piece(i)], sem.at[0, i, 0]))
            copies.append(pltpu.make_async_copy(new_dn.at[dn_piece(i), :], dn_out.at[dn_piece(i), :], sem.at[1, i, 0]))
        for c in copies:
            c.start()
        y_v[0] = jnp.zeros_like(y_v[0])
        ys = [pltpu.make_async_copy(y_v.at[0], y_piece(i), y_sem.at[i]) for i in range(blocks)]
        for c in ys:
            c.start()
        for c in copies + ys:
            c.wait()

    @pl.when(side == 1)
    def generator():
        last = land_up.shape[0] - 1
        landed = pltpu.make_async_copy(land_up.at[last], lb_up, l_sem.at[0])
        landed.start()
        size = zero.shape[1]
        copies = []
        for i in range(n):
            for j in range(pieces):
                copies.append(pltpu.make_async_copy(
                    zero, up_out.at[:, pl.ds(i * width + j * size, size)], sem.at[0, i, j]))
                copies.append(pltpu.make_async_copy(
                    zero, dn_out.at[pl.ds(i * rows_dn + j * depth, depth), :], sem.at[1, i, j]))
        for c in copies:
            c.start()
        for k in range(2):
            ks = pl.ds(k * COLS, COLS)
            for r in range(4):
                cols = pl.ds(r * depth, depth)
                wg[ks, cols] = (sb_dn[k, :, cols].astype(jnp.float32) + last_dn[r, ks, :].astype(jnp.float32)).astype(jnp.bfloat16)
        landed.wait()
        for r in range(4):
            rows = pl.ds(r * depth, depth)
            wg_up[rows, :] = (sb_up[last % 2, rows, :].astype(jnp.float32) + lb_up[r].astype(jnp.float32)).astype(jnp.bfloat16)

        def up(i, _):
            rows = pl.ds(pl.multiple_of(i * TILE, TILE), TILE)
            pre = jnp.dot(x_v[rows, :], wg_up[...], preferred_element_type=jnp.float32)
            u_last[rows, :] = gelu(pre).astype(jnp.bfloat16)
            return 0
        lax.fori_loop(0, tokens // TILE, up, 0)

        def out(i):
            return pltpu.make_async_copy(y_v.at[i], y_out.at[pl.ds(pl.multiple_of(i * depth, depth), depth), :], y_sem.at[i])

        def block(i, _):
            rows = pl.ds(pl.multiple_of(i * depth, depth), depth)
            cols = pl.ds(pl.multiple_of(i * width, width), width)
            u = jnp.concatenate([u_v[rows, :COLS], u_last[rows, :]], axis=1)
            p = jnp.dot(u, wg[...], preferred_element_type=jnp.float32)
            y_v[i] = (acc[:, cols] + p).astype(jnp.bfloat16)

            @pl.when(i >= 1)
            def _():
                out(i - 1).start()
            return 0
        lax.fori_loop(0, blocks, block, 0)
        for c in copies[:len(copies) // 2]:
            c.wait()
        out(blocks - 1).start()
        for c in copies[len(copies) // 2:]:
            c.wait()
        for i in range(blocks):
            out(i).wait()


def step_outputs(lr, w_up, w_dn, g_up, g_dn, s_up, s_dn, x):
    depth, hid = w_up.shape
    tokens, width = x.shape
    chunks = hid // COLS
    any_spec = pl.BlockSpec(memory_space=pltpu.HBM)
    vmem_spec = pl.BlockSpec(memory_space=pltpu.VMEM)
    dma = pltpu.SemaphoreType.DMA
    vmem = pltpu.VMEM
    f32, bf16 = jnp.float32, jnp.bfloat16
    land_up, _, *held = pl.pallas_call(
        sync_kernel,
        name="sync_kernel",
        out_shape=(
            jax.ShapeDtypeStruct((chunks, 4, depth, COLS), bf16),
            jax.ShapeDtypeStruct((chunks, 4, COLS, depth), bf16),
            vmem((tokens, width), bf16),
            vmem(w_up.shape, f32),
            vmem(w_dn.shape, f32),
            vmem((tokens, 2 * COLS), bf16),
            vmem((2, width, COLS), bf16),
            vmem((2, COLS, width), bf16),
            vmem((4, 2 * COLS, depth), bf16),
            vmem((depth, depth), f32),
        ),
        in_specs=[any_spec] * 8,
        out_specs=(any_spec,) * 2 + (vmem_spec,) * 8,
        scratch_shapes=[
            vmem((2, depth, COLS), f32), vmem((2, COLS, depth), f32),
            vmem((2, depth, COLS), f32), vmem((2, COLS, depth), f32),
            vmem((SENDS, depth, COLS), bf16), vmem((SENDS, COLS, depth), bf16),
            vmem((HALF, depth), bf16),
            vmem((4, depth, COLS), bf16), vmem((4, COLS, depth), bf16),
            vmem((width, COLS), bf16), vmem((COLS, width), bf16),
            pltpu.SMEM((1,), f32), dma((4, 2)), dma((2, SENDS)), dma((2, 2)), dma((2,)), dma((1,)),
        ] + [dma((2, chunks))] * 7 + [dma((5,))] * 7 + [dma((2,))],
        compiler_params=pltpu.CompilerParams(
            collective_id=0, has_side_effects=True, vmem_limit_bytes=VMEM_SYNC),
        cost_estimate=pl.CostEstimate(flops=4 * tokens * width * hid, bytes_accessed=8 * width * hid, transcendentals=0),
    )(lr, w_up, w_dn, g_up, g_dn, s_up, s_dn, x)
    n = hid // width
    return pl.pallas_call(
        finish_kernel,
        name="finish_kernel",
        out_shape=(
            jax.ShapeDtypeStruct(w_up.shape, f32),
            jax.ShapeDtypeStruct(w_dn.shape, f32),
            jax.ShapeDtypeStruct((tokens, width), bf16),
        ),
        in_specs=[vmem_spec] * 8 + [any_spec],
        out_specs=(any_spec,) * 3,
        scratch_shapes=[
            vmem((width, COLS), bf16), vmem((2 * COLS, width), bf16),
            vmem((tokens // depth, depth, width), bf16),
            vmem((tokens, COLS), bf16), vmem((4, depth, COLS), bf16),
            dma((2, n, width // depth)), dma((tokens // depth,)), dma((1,)),
        ],
        compiler_params=pltpu.CompilerParams(vmem_limit_bytes=VMEM_FINISH),
        cost_estimate=pl.CostEstimate(flops=4 * tokens * width * COLS, bytes_accessed=12 * depth * hid, transcendentals=0),
    )(*[pltpu.with_memory_space_constraint(a, pltpu.VMEM) for a in held], land_up)


def solution(mesh):
    up_spec = P("side", None, "rep", None)
    down_spec = P("side", None, None, "rep")
    copy_spec = P("side", "rep", None, None, None)
    token_spec = P("side", "rep", None, None)

    def local_step(w_up, w_down, g_up, g_down, learn_rate, old_up, old_down, prompts):
        new_up, new_down, y = step_outputs(
            learn_rate, w_up[0, 0], w_down[0, 0], g_up[0, 0], g_down[0, 0],
            old_up[0, 0, 0], old_down[0, 0, 0], prompts[0, 0])
        return new_up[None, None], new_down[None, None], y[None, None]

    return jax.shard_map(
        local_step,
        mesh=mesh,
        in_specs=(up_spec, down_spec, up_spec, down_spec, P(None), copy_spec, copy_spec, token_spec),
        out_specs=(up_spec, down_spec, token_spec),
        check_vma=False,
    )
```

```python
import functools

import jax
import jax.numpy as jnp
from jax import lax
from jax.experimental import pallas as pl
from jax.experimental.pallas import tpu as pltpu
from jax.sharding import PartitionSpec as P

MESH = pl.DeviceIdType.MESH
COLS = 256
SENDS = 4
TILE = 1024
HALF = COLS // 2
SWAP = 160
VMEM_SYNC = 14 * 1024 * 1024
VMEM_FINISH = 14 * 1024 * 1024


def gelu(x):
    return 0.5 * x * (1.0 + lax.erf(x * 0.7071067811865476))


def sync_kernel(lr_hbm, w_up, w_dn, g_up, g_dn, s_up, s_dn, x_hbm,
                land_up, land_dn, x_v, acc, new_dn, u_v, sb_up, sb_dn, last_dn, zero,
                wb_up, wb_dn, gb_up, gb_dn, d_up, d_dn, swap_dn, lb_up, lb_dn, wg_up, wg_dn,
                lr, t_sem, send_sem, s_sem, l_sem, x_sem,
                y_recv, x_recv, o_recv, n_recv, x_send, o_send, n_send,
                yt_recv, xt_recv, ot_recv, nt_recv, xt_send, ot_send, nt_send, swap_sem):
    side, rep = lax.axis_index("side"), lax.axis_index("rep")
    other = 1 - side
    sib = rep + 1 - 2 * (rep % 2)
    cross = (rep + 2) % 4
    sib_cross = (sib + 2) % 4
    chunks = land_up.shape[0]
    depth = w_up.shape[0]
    tokens, width = x_v.shape
    lands, smalls = (land_up, land_dn), (d_up, d_dn)
    last = chunks - 1

    barrier = pltpu.get_barrier_semaphore()
    for dev in ((other, rep), (side, sib), (side, cross)):
        pl.semaphore_signal(barrier, inc=1, device_id=dev, device_id_type=MESH)

    def span(m):
        return pl.ds(pl.multiple_of(m * COLS, COLS), COLS)

    def swapped(row):
        return last_dn.at[row, pl.ds(2 * COLS - SWAP, SWAP), :]

    def late(row, q):
        return last_dn.at[row, pl.ds(q * HALF, HALF), :]

    @pl.when(side == 0)
    def trainer():
        mats = ((w_up, g_up, wb_up, gb_up), (w_dn, g_dn, wb_dn, gb_dn))

        def part(h, ref, m):
            return ref.at[:, span(m)] if h == 0 else ref.at[span(m), :]

        def loads(h, m):
            w, g, wb, gb = mats[h]
            k = m % 2
            return [
                pltpu.make_async_copy(part(h, w, m), wb.at[k], t_sem.at[2 * h, k]),
                pltpu.make_async_copy(part(h, g, m), gb.at[k], t_sem.at[2 * h + 1, k]),
            ]

        def send(h, m):
            return pltpu.make_async_remote_copy(
                src_ref=smalls[h].at[m % SENDS], dst_ref=lands[h].at[m, rep],
                send_sem=send_sem.at[h, m % SENDS], recv_sem=y_recv.at[h, m],
                device_id=(other, rep), device_id_type=MESH)

        def send_late(q):
            m = last - 1 + q // 2
            return pltpu.make_async_remote_copy(
                src_ref=d_dn.at[m % SENDS, pl.ds((q % 2) * HALF, HALF), :], dst_ref=late(rep, q),
                send_sem=xt_send.at[q], recv_sem=yt_recv.at[q],
                device_id=(other, rep), device_id_type=MESH)

        swap = pltpu.make_async_remote_copy(
            src_ref=d_dn.at[last % SENDS, pl.ds(COLS - SWAP, SWAP), :], dst_ref=swap_dn,
            send_sem=swap_sem.at[0], recv_sem=swap_sem.at[1],
            device_id=(side, cross), device_id_type=MESH)
        send_swapped = pltpu.make_async_remote_copy(
            src_ref=swap_dn, dst_ref=swapped(cross),
            send_sem=xt_send.at[4], recv_sem=yt_recv.at[4],
            device_id=(other, rep), device_id_type=MESH)

        lr_in = pltpu.make_async_copy(lr_hbm, lr, x_sem.at[0])
        lr_in.start()
        for c in loads(0, 0):
            c.start()
        lr_in.wait()
        rate = lr[0]

        def make(h, m):
            k = m % 2
            for c in loads(h, m):
                c.wait()

            @pl.when(m >= SENDS)
            def _():
                send(h, m - SENDS).wait_send()
            old = mats[h][2][k]
            new = old - rate * mats[h][3][k]
            if h == 0:
                acc[:, span(m)] = new
            else:
                new_dn[span(m), :] = new
            smalls[h][m % SENDS] = (new - old).astype(jnp.bfloat16)

            @pl.when(m + 2 < chunks)
            def _():
                for c in loads(h, m + 2):
                    c.start()

        make(0, 0)
        for h, m in ((0, 1), (1, 0), (1, 1)):
            for c in loads(h, m):
                c.start()
        pl.semaphore_wait(barrier, 3)
        send(0, 0).start()

        def step(m, _):
            make(0, m + 1)

            @pl.when(m >= 1)
            def _():
                send(1, m - 1).start()
            make(1, m)
            send(0, m + 1).start()
            return 0

        lax.fori_loop(0, last, step, 0)
        make(1, last)
        for q in range(4):
            send_late(q).start()
        swap.start()
        swap.wait_recv()
        send_swapped.start()
        swap.wait_send()
        for m in range(chunks - SENDS, chunks):
            send(0, m).wait_send()
        for m in range(chunks - SENDS, last - 1):
            send(1, m).wait_send()
        for q in range(4):
            send_late(q).wait_send()
        send_swapped.wait_send()

    @pl.when(side == 1)
    def generator():
        def hop(h, m, row, dev, send, recv):
            return pltpu.make_async_remote_copy(
                src_ref=lands[h].at[m, row], dst_ref=lands[h].at[m, row],
                send_sem=send.at[h, m], recv_sem=recv.at[h, m],
                device_id=(side, dev), device_id_type=MESH)

        def from_trainer(h, m):
            return hop(h, m, rep, sib, x_send, y_recv)

        def across(h, m, row):
            return hop(h, m, row, cross, x_send, x_recv)

        def own(h, m, row):
            return hop(h, m, row, sib, o_send, o_recv)

        def next_own(h, m, row):
            return hop(h, m, row, sib, n_send, n_recv)

        def cross_part(q):
            first = q * HALF if q < 3 else 2 * COLS - SWAP
            return pl.ds(first, min(HALF, 2 * COLS - SWAP - first) if q < 3 else SWAP)

        def cross_hop(q, row, dev, send, recv):
            ref = last_dn.at[row, cross_part(q), :]
            return pltpu.make_async_remote_copy(
                src_ref=ref, dst_ref=ref, send_sem=send.at[q], recv_sem=recv.at[q],
                device_id=(side, dev), device_id_type=MESH)

        def late_hop(q, row, dev, send, recv):
            return pltpu.make_async_remote_copy(
                src_ref=late(row, q), dst_ref=late(row, q), send_sem=send.at[q], recv_sem=recv.at[q],
                device_id=(side, dev), device_id_type=MESH)

        stales = (sb_up, sb_dn)

        def stale(h, m):
            src = s_up.at[:, span(m)] if h == 0 else s_dn.at[span(m), :]
            return pltpu.make_async_copy(src, stales[h].at[m % 2], s_sem.at[h, m % 2])

        def landed(h, m):
            return pltpu.make_async_copy(lands[h].at[m], (lb_up, lb_dn)[h], l_sem.at[h])

        x_in = pltpu.make_async_copy(x_hbm, x_v, x_sem.at[0])
        x_in.start()
        for m in range(2):
            for h in range(2):
                stale(h, m).start()
        pl.semaphore_wait(barrier, 3)

        def pass_on(h, m):
            from_trainer(h, m).wait_recv()
            across(h, m, rep).start()
            own(h, m, rep).start()

        def pass_late(q):
            late_hop(q, rep, sib, xt_send, yt_recv).wait_recv()
            if q < 3:
                cross_hop(q, rep, cross, xt_send, xt_recv).start()
            late_hop(q, rep, sib, ot_send, ot_recv).start()

        def turn(h, m):
            across(h, m, cross).wait_recv()
            next_own(h, m, cross).start()

        def turn_late(q):
            if q < 3:
                cross_hop(q, cross, cross, xt_send, xt_recv).wait_recv()
            else:
                pltpu.make_async_remote_copy(
                    src_ref=swapped(cross), dst_ref=swapped(cross), send_sem=xt_send.at[4], recv_sem=yt_recv.at[4],
                    device_id=(side, sib), device_id_type=MESH).wait_recv()
            cross_hop(q, cross, sib, nt_send, nt_recv).start()

        def fetch(h, m):
            own(h, m, sib).wait_recv()
            next_own(h, m, sib_cross).wait_recv()
            landed(h, m).start()

        tiles = tokens // TILE
        groups = TILE // depth

        def tile_rows(i):
            return pl.ds(pl.multiple_of(i * TILE, TILE), TILE)

        def u_cols(m):
            return pl.ds(pl.multiple_of((m % 2) * COLS, COLS), COLS)

        def up(m):
            k = m % 2
            stale(0, m).wait()
            landed(0, m).wait()
            for r in range(4):
                rows = pl.ds(r * depth, depth)
                wg_up[rows, :] = (sb_up[k, rows, :].astype(jnp.float32) + lb_up[r].astype(jnp.float32)).astype(jnp.bfloat16)

            @pl.when(m + 2 < chunks)
            def _():
                stale(0, m + 2).start()

            def tile(i, _):
                pre = jnp.dot(x_v[tile_rows(i), :], wg_up[...], preferred_element_type=jnp.float32)
                u_v[tile_rows(i), u_cols(m)] = gelu(pre).astype(jnp.bfloat16)
                return 0
            lax.fori_loop(0, tiles, tile, 0)

        def down(m):
            k = m % 2
            stale(1, m).wait()
            landed(1, m).wait()
            for r in range(4):
                cols = pl.ds(r * depth, depth)
                wg_dn[:, cols] = (sb_dn[k, :, cols].astype(jnp.float32) + lb_dn[r].astype(jnp.float32)).astype(jnp.bfloat16)

            @pl.when(m + 2 < chunks)
            def _():
                stale(1, m + 2).start()

            def tile(i, _):
                p = jnp.dot(u_v[tile_rows(i), u_cols(m)], wg_dn[...], preferred_element_type=jnp.float32)
                for g in range(groups):
                    cols = pl.ds(pl.multiple_of((i * groups + g) * width, width), width)
                    acc[:, cols] += p[g * depth:(g + 1) * depth]
                return 0
            lax.fori_loop(0, tiles, tile, 0)

        pass_on(0, 0)
        x_in.wait()
        zero[...] = jnp.zeros_like(zero)

        def clear(i, _):
            cols = pl.ds(pl.multiple_of(i * width, width), width)
            rows = pl.ds(pl.multiple_of(i * depth, depth), depth)
            acc[:, cols] = x_v[rows, :].astype(jnp.float32)
            return 0
        lax.fori_loop(0, tokens // depth, clear, 0)

        def step(m, _):
            pass_on(0, m)
            turn(0, m - 1)

            @pl.when(m >= 3)
            def _():
                down(m - 3)
            fetch(0, m - 1)
            pass_on(1, m - 1)

            @pl.when(m >= 2)
            def _():
                turn(1, m - 2)
            up(m - 1)

            @pl.when(m >= 2)
            def _():
                fetch(1, m - 2)
            return 0

        lax.fori_loop(1, last, step, 0)
        pass_on(0, last)
        turn(0, last - 1)
        down(last - 3)
        fetch(0, last - 1)
        pass_late(0)
        turn(1, last - 2)
        up(last - 1)
        pass_late(1)
        fetch(1, last - 2)
        turn(0, last)
        pass_late(2)
        down(last - 2)
        pass_late(3)
        for q in range(4):
            turn_late(q)
        stale(0, last).wait()
        for m in range(last - 1, chunks):
            stale(1, m).wait()
        own(0, last, sib).wait_recv()
        next_own(0, last, sib_cross).wait_recv()

        def drain(m, _):
            across(0, m, rep).wait_send()
            own(0, m, rep).wait_send()
            next_own(0, m, cross).wait_send()

            @pl.when(m < last - 1)
            def _():
                across(1, m, rep).wait_send()
                own(1, m, rep).wait_send()
                next_own(1, m, cross).wait_send()
            return 0
        lax.fori_loop(0, chunks, drain, 0)
        for q in range(4):
            late_hop(q, sib, sib, ot_send, ot_recv).wait_recv()
            cross_hop(q, sib_cross, sib, nt_send, nt_recv).wait_recv()
        for q in range(4):
            if q < 3:
                cross_hop(q, rep, cross, xt_send, xt_recv).wait_send()
            late_hop(q, rep, sib, ot_send, ot_recv).wait_send()
            cross_hop(q, cross, sib, nt_send, nt_recv).wait_send()


def finish_kernel(x_v, acc, new_dn, u_v, sb_up, sb_dn, last_dn, zero, land_up, up_out, dn_out, y_out,
                  wg_up, wg, y_v, u_last, lb_up, sem, y_sem, l_sem):
    side = lax.axis_index("side")
    depth = acc.shape[0]
    tokens, width = x_v.shape
    n = up_out.shape[1] // width
    rows_dn = dn_out.shape[0] // n
    blocks = tokens // depth
    pieces = width // zero.shape[1]

    def up_piece(i):
        return pl.ds(i * width, width)

    def dn_piece(i):
        return pl.ds(i * rows_dn, rows_dn)

    def y_piece(i):
        return y_out.at[pl.ds(i * depth, depth), :]

    @pl.when(side == 0)
    def trainer():
        copies = []
        for i in range(n):
            copies.append(pltpu.make_async_copy(acc.at[:, up_piece(i)], up_out.at[:, up_piece(i)], sem.at[0, i, 0]))
            copies.append(pltpu.make_async_copy(new_dn.at[dn_piece(i), :], dn_out.at[dn_piece(i), :], sem.at[1, i, 0]))
        for c in copies:
            c.start()
        y_v[0] = jnp.zeros_like(y_v[0])
        ys = [pltpu.make_async_copy(y_v.at[0], y_piece(i), y_sem.at[i]) for i in range(blocks)]
        for c in ys:
            c.start()
        for c in copies + ys:
            c.wait()

    @pl.when(side == 1)
    def generator():
        last = land_up.shape[0] - 1
        landed = pltpu.make_async_copy(land_up.at[last], lb_up, l_sem.at[0])
        landed.start()
        size = zero.shape[1]
        copies = []
        for i in range(n):
            for j in range(pieces):
                copies.append(pltpu.make_async_copy(
                    zero, up_out.at[:, pl.ds(i * width + j * size, size)], sem.at[0, i, j]))
                copies.append(pltpu.make_async_copy(
                    zero, dn_out.at[pl.ds(i * rows_dn + j * depth, depth), :], sem.at[1, i, j]))
        for c in copies:
            c.start()
        for k in range(2):
            ks = pl.ds(k * COLS, COLS)
            for r in range(4):
                cols = pl.ds(r * depth, depth)
                wg[ks, cols] = (sb_dn[k, :, cols].astype(jnp.float32) + last_dn[r, ks, :].astype(jnp.float32)).astype(jnp.bfloat16)
        landed.wait()
        for r in range(4):
            rows = pl.ds(r * depth, depth)
            wg_up[rows, :] = (sb_up[last % 2, rows, :].astype(jnp.float32) + lb_up[r].astype(jnp.float32)).astype(jnp.bfloat16)

        def up(i, _):
            rows = pl.ds(pl.multiple_of(i * TILE, TILE), TILE)
            pre = jnp.dot(x_v[rows, :], wg_up[...], preferred_element_type=jnp.float32)
            u_last[rows, :] = gelu(pre).astype(jnp.bfloat16)
            return 0
        lax.fori_loop(0, tokens // TILE, up, 0)

        def out(i):
            return pltpu.make_async_copy(y_v.at[i], y_out.at[pl.ds(pl.multiple_of(i * depth, depth), depth), :], y_sem.at[i])

        def block(i, _):
            rows = pl.ds(pl.multiple_of(i * depth, depth), depth)
            cols = pl.ds(pl.multiple_of(i * width, width), width)
            u = jnp.concatenate([u_v[rows, :COLS], u_last[rows, :]], axis=1)
            p = jnp.dot(u, wg[...], preferred_element_type=jnp.float32)
            y_v[i] = (acc[:, cols] + p).astype(jnp.bfloat16)

            @pl.when(i >= 1)
            def _():
                out(i - 1).start()
            return 0
        lax.fori_loop(0, blocks, block, 0)
        for c in copies[:len(copies) // 2]:
            c.wait()
        out(blocks - 1).start()
        for c in copies[len(copies) // 2:]:
            c.wait()
        for i in range(blocks):
            out(i).wait()


def step_outputs(lr, w_up, w_dn, g_up, g_dn, s_up, s_dn, x):
    depth, hid = w_up.shape
    tokens, width = x.shape
    chunks = hid // COLS
    any_spec = pl.BlockSpec(memory_space=pltpu.HBM)
    vmem_spec = pl.BlockSpec(memory_space=pltpu.VMEM)
    dma = pltpu.SemaphoreType.DMA
    vmem = pltpu.VMEM
    f32, bf16 = jnp.float32, jnp.bfloat16
    land_up, _, *held = pl.pallas_call(
        sync_kernel,
        name="sync_kernel",
        out_shape=(
            jax.ShapeDtypeStruct((chunks, 4, depth, COLS), bf16),
            jax.ShapeDtypeStruct((chunks, 4, COLS, depth), bf16),
            vmem((tokens, width), bf16),
            vmem(w_up.shape, f32),
            vmem(w_dn.shape, f32),
            vmem((tokens, 2 * COLS), bf16),
            vmem((2, width, COLS), bf16),
            vmem((2, COLS, width), bf16),
            vmem((4, 2 * COLS, depth), bf16),
            vmem((depth, depth), f32),
        ),
        in_specs=[any_spec] * 8,
        out_specs=(any_spec,) * 2 + (vmem_spec,) * 8,
        scratch_shapes=[
            vmem((2, depth, COLS), f32), vmem((2, COLS, depth), f32),
            vmem((2, depth, COLS), f32), vmem((2, COLS, depth), f32),
            vmem((SENDS, depth, COLS), bf16), vmem((SENDS, COLS, depth), bf16),
            vmem((SWAP, depth), bf16),
            vmem((4, depth, COLS), bf16), vmem((4, COLS, depth), bf16),
            vmem((width, COLS), bf16), vmem((COLS, width), bf16),
            pltpu.SMEM((1,), f32), dma((4, 2)), dma((2, SENDS)), dma((2, 2)), dma((2,)), dma((1,)),
        ] + [dma((2, chunks))] * 7 + [dma((5,))] * 7 + [dma((2,))],
        compiler_params=pltpu.CompilerParams(
            collective_id=0, has_side_effects=True, vmem_limit_bytes=VMEM_SYNC),
        cost_estimate=pl.CostEstimate(flops=4 * tokens * width * hid, bytes_accessed=8 * width * hid, transcendentals=0),
    )(lr, w_up, w_dn, g_up, g_dn, s_up, s_dn, x)
    n = hid // width
    return pl.pallas_call(
        finish_kernel,
        name="finish_kernel",
        out_shape=(
            jax.ShapeDtypeStruct(w_up.shape, f32),
            jax.ShapeDtypeStruct(w_dn.shape, f32),
            jax.ShapeDtypeStruct((tokens, width), bf16),
        ),
        in_specs=[vmem_spec] * 8 + [any_spec],
        out_specs=(any_spec,) * 3,
        scratch_shapes=[
            vmem((width, COLS), bf16), vmem((2 * COLS, width), bf16),
            vmem((tokens // depth, depth, width), bf16),
            vmem((tokens, COLS), bf16), vmem((4, depth, COLS), bf16),
            dma((2, n, width // depth)), dma((tokens // depth,)), dma((1,)),
        ],
        compiler_params=pltpu.CompilerParams(vmem_limit_bytes=VMEM_FINISH),
        cost_estimate=pl.CostEstimate(flops=4 * tokens * width * COLS, bytes_accessed=12 * depth * hid, transcendentals=0),
    )(*[pltpu.with_memory_space_constraint(a, pltpu.VMEM) for a in held], land_up)


def solution(mesh):
    up_spec = P("side", None, "rep", None)
    down_spec = P("side", None, None, "rep")
    copy_spec = P("side", "rep", None, None, None)
    token_spec = P("side", "rep", None, None)

    def local_step(w_up, w_down, g_up, g_down, learn_rate, old_up, old_down, prompts):
        new_up, new_down, y = step_outputs(
            learn_rate, w_up[0, 0], w_down[0, 0], g_up[0, 0], g_down[0, 0],
            old_up[0, 0, 0], old_down[0, 0, 0], prompts[0, 0])
        return new_up[None, None], new_down[None, None], y[None, None]

    return jax.shard_map(
        local_step,
        mesh=mesh,
        in_specs=(up_spec, down_spec, up_spec, down_spec, P(None), copy_spec, copy_spec, token_spec),
        out_specs=(up_spec, down_spec, token_spec),
        check_vma=False,
    )
```

```python
import functools

import jax
import jax.numpy as jnp
from jax import lax
from jax.experimental import pallas as pl
from jax.experimental.pallas import tpu as pltpu
from jax.sharding import PartitionSpec as P

MESH = pl.DeviceIdType.MESH
COLS = 256
SENDS = 4
TILE = 1024
HALF = COLS // 2
SWAP = 160
VMEM_SYNC = 14 * 1024 * 1024
VMEM_FINISH = 14 * 1024 * 1024


def gelu(x):
    return 0.5 * x * (1.0 + lax.erf(x * 0.7071067811865476))


def sync_kernel(lr_hbm, w_up, w_dn, g_up, g_dn, s_up, s_dn, x_hbm,
                land_up, land_dn, x_v, acc, new_dn, u_v, sb_up, sb_dn, last_dn, zero,
                wb_up, wb_dn, gb_up, gb_dn, d_up, d_dn, swap_dn, lb_up, lb_dn, wg_up, wg_dn,
                lr, t_sem, send_sem, s_sem, l_sem, x_sem,
                y_recv, x_recv, o_recv, n_recv, x_send, o_send, n_send,
                yt_recv, xt_recv, ot_recv, nt_recv, xt_send, ot_send, nt_send, swap_sem):
    side, rep = lax.axis_index("side"), lax.axis_index("rep")
    other = 1 - side
    sib = rep + 1 - 2 * (rep % 2)
    cross = (rep + 2) % 4
    sib_cross = (sib + 2) % 4
    chunks = land_up.shape[0]
    depth = w_up.shape[0]
    tokens, width = x_v.shape
    lands, smalls = (land_up, land_dn), (d_up, d_dn)
    last = chunks - 1

    barrier = pltpu.get_barrier_semaphore()
    for dev in ((other, rep), (side, sib), (side, cross)):
        pl.semaphore_signal(barrier, inc=1, device_id=dev, device_id_type=MESH)

    def span(m):
        return pl.ds(pl.multiple_of(m * COLS, COLS), COLS)

    def swapped(row):
        return last_dn.at[row, pl.ds(2 * COLS - SWAP, SWAP), :]

    def late(row, q):
        return last_dn.at[row, pl.ds(q * HALF, HALF), :]

    @pl.when(side == 0)
    def trainer():
        mats = ((w_up, g_up, wb_up, gb_up), (w_dn, g_dn, wb_dn, gb_dn))

        def part(h, ref, m):
            return ref.at[:, span(m)] if h == 0 else ref.at[span(m), :]

        def loads(h, m):
            w, g, wb, gb = mats[h]
            k = m % 2
            return [
                pltpu.make_async_copy(part(h, w, m), wb.at[k], t_sem.at[2 * h, k]),
                pltpu.make_async_copy(part(h, g, m), gb.at[k], t_sem.at[2 * h + 1, k]),
            ]

        def send(h, m):
            return pltpu.make_async_remote_copy(
                src_ref=smalls[h].at[m % SENDS], dst_ref=lands[h].at[m, rep],
                send_sem=send_sem.at[h, m % SENDS], recv_sem=y_recv.at[h, m],
                device_id=(other, rep), device_id_type=MESH)

        def send_late(q):
            m = last - 1 + q // 2
            return pltpu.make_async_remote_copy(
                src_ref=d_dn.at[m % SENDS, pl.ds((q % 2) * HALF, HALF), :], dst_ref=late(rep, q),
                send_sem=xt_send.at[q], recv_sem=yt_recv.at[q],
                device_id=(other, rep), device_id_type=MESH)

        swap = pltpu.make_async_remote_copy(
            src_ref=d_dn.at[last % SENDS, pl.ds(COLS - SWAP, SWAP), :], dst_ref=swap_dn,
            send_sem=swap_sem.at[0], recv_sem=swap_sem.at[1],
            device_id=(side, cross), device_id_type=MESH)
        send_swapped = pltpu.make_async_remote_copy(
            src_ref=swap_dn, dst_ref=swapped(cross),
            send_sem=xt_send.at[4], recv_sem=yt_recv.at[4],
            device_id=(other, rep), device_id_type=MESH)

        lr_in = pltpu.make_async_copy(lr_hbm, lr, x_sem.at[0])
        lr_in.start()
        for c in loads(0, 0):
            c.start()
        lr_in.wait()
        rate = lr[0]

        def make(h, m):
            k = m % 2
            for c in loads(h, m):
                c.wait()

            @pl.when(m >= SENDS)
            def _():
                send(h, m - SENDS).wait_send()
            old = mats[h][2][k]
            new = old - rate * mats[h][3][k]
            if h == 0:
                acc[:, span(m)] = new
            else:
                new_dn[span(m), :] = new
            smalls[h][m % SENDS] = (new - old).astype(jnp.bfloat16)

            @pl.when(m + 2 < chunks)
            def _():
                for c in loads(h, m + 2):
                    c.start()

        make(0, 0)
        for h, m in ((0, 1), (1, 0), (1, 1)):
            for c in loads(h, m):
                c.start()
        pl.semaphore_wait(barrier, 3)
        send(0, 0).start()

        def step(m, _):
            make(0, m + 1)

            @pl.when(m >= 1)
            def _():
                send(1, m - 1).start()
            make(1, m)
            send(0, m + 1).start()
            return 0

        lax.fori_loop(0, last, step, 0)
        make(1, last)
        for q in range(4):
            send_late(q).start()
        for h in range(2):
            send(h, chunks - SENDS).wait_send()
        swap.start()
        swap.wait_recv()
        send_swapped.start()
        swap.wait_send()
        for m in range(chunks - SENDS + 1, chunks):
            send(0, m).wait_send()
        for m in range(chunks - SENDS + 1, last - 1):
            send(1, m).wait_send()
        for q in range(4):
            send_late(q).wait_send()
        send_swapped.wait_send()

    @pl.when(side == 1)
    def generator():
        def hop(h, m, row, dev, send, recv):
            return pltpu.make_async_remote_copy(
                src_ref=lands[h].at[m, row], dst_ref=lands[h].at[m, row],
                send_sem=send.at[h, m], recv_sem=recv.at[h, m],
                device_id=(side, dev), device_id_type=MESH)

        def from_trainer(h, m):
            return hop(h, m, rep, sib, x_send, y_recv)

        def across(h, m, row):
            return hop(h, m, row, cross, x_send, x_recv)

        def own(h, m, row):
            return hop(h, m, row, sib, o_send, o_recv)

        def next_own(h, m, row):
            return hop(h, m, row, sib, n_send, n_recv)

        def cross_part(q):
            first = q * HALF if q < 3 else 2 * COLS - SWAP
            return pl.ds(first, min(HALF, 2 * COLS - SWAP - first) if q < 3 else SWAP)

        def cross_hop(q, row, dev, send, recv):
            ref = last_dn.at[row, cross_part(q), :]
            return pltpu.make_async_remote_copy(
                src_ref=ref, dst_ref=ref, send_sem=send.at[q], recv_sem=recv.at[q],
                device_id=(side, dev), device_id_type=MESH)

        def late_hop(q, row, dev, send, recv):
            return pltpu.make_async_remote_copy(
                src_ref=late(row, q), dst_ref=late(row, q), send_sem=send.at[q], recv_sem=recv.at[q],
                device_id=(side, dev), device_id_type=MESH)

        stales = (sb_up, sb_dn)

        def stale(h, m):
            src = s_up.at[:, span(m)] if h == 0 else s_dn.at[span(m), :]
            return pltpu.make_async_copy(src, stales[h].at[m % 2], s_sem.at[h, m % 2])

        def landed(h, m):
            return pltpu.make_async_copy(lands[h].at[m], (lb_up, lb_dn)[h], l_sem.at[h])

        x_in = pltpu.make_async_copy(x_hbm, x_v, x_sem.at[0])
        x_in.start()
        for m in range(2):
            for h in range(2):
                stale(h, m).start()
        pl.semaphore_wait(barrier, 3)

        def pass_on(h, m):
            from_trainer(h, m).wait_recv()
            across(h, m, rep).start()
            own(h, m, rep).start()

        def pass_late(q):
            late_hop(q, rep, sib, xt_send, yt_recv).wait_recv()
            if q < 3:
                cross_hop(q, rep, cross, xt_send, xt_recv).start()
            late_hop(q, rep, sib, ot_send, ot_recv).start()

        def turn(h, m):
            across(h, m, cross).wait_recv()
            next_own(h, m, cross).start()

        def turn_late(q):
            if q < 3:
                cross_hop(q, cross, cross, xt_send, xt_recv).wait_recv()
            else:
                pltpu.make_async_remote_copy(
                    src_ref=swapped(cross), dst_ref=swapped(cross), send_sem=xt_send.at[4], recv_sem=yt_recv.at[4],
                    device_id=(side, sib), device_id_type=MESH).wait_recv()
            cross_hop(q, cross, sib, nt_send, nt_recv).start()

        def fetch(h, m):
            own(h, m, sib).wait_recv()
            next_own(h, m, sib_cross).wait_recv()
            landed(h, m).start()

        tiles = tokens // TILE
        groups = TILE // depth

        def tile_rows(i):
            return pl.ds(pl.multiple_of(i * TILE, TILE), TILE)

        def u_cols(m):
            return pl.ds(pl.multiple_of((m % 2) * COLS, COLS), COLS)

        def up(m):
            k = m % 2
            stale(0, m).wait()
            landed(0, m).wait()
            for r in range(4):
                rows = pl.ds(r * depth, depth)
                wg_up[rows, :] = (sb_up[k, rows, :].astype(jnp.float32) + lb_up[r].astype(jnp.float32)).astype(jnp.bfloat16)

            @pl.when(m + 2 < chunks)
            def _():
                stale(0, m + 2).start()

            def tile(i, _):
                pre = jnp.dot(x_v[tile_rows(i), :], wg_up[...], preferred_element_type=jnp.float32)
                u_v[tile_rows(i), u_cols(m)] = gelu(pre).astype(jnp.bfloat16)
                return 0
            lax.fori_loop(0, tiles, tile, 0)

        def down(m):
            k = m % 2
            stale(1, m).wait()
            landed(1, m).wait()
            for r in range(4):
                cols = pl.ds(r * depth, depth)
                wg_dn[:, cols] = (sb_dn[k, :, cols].astype(jnp.float32) + lb_dn[r].astype(jnp.float32)).astype(jnp.bfloat16)

            @pl.when(m + 2 < chunks)
            def _():
                stale(1, m + 2).start()

            def tile(i, _):
                p = jnp.dot(u_v[tile_rows(i), u_cols(m)], wg_dn[...], preferred_element_type=jnp.float32)
                for g in range(groups):
                    cols = pl.ds(pl.multiple_of((i * groups + g) * width, width), width)
                    acc[:, cols] += p[g * depth:(g + 1) * depth]
                return 0
            lax.fori_loop(0, tiles, tile, 0)

        pass_on(0, 0)
        x_in.wait()
        zero[...] = jnp.zeros_like(zero)

        def clear(i, _):
            cols = pl.ds(pl.multiple_of(i * width, width), width)
            rows = pl.ds(pl.multiple_of(i * depth, depth), depth)
            acc[:, cols] = x_v[rows, :].astype(jnp.float32)
            return 0
        lax.fori_loop(0, tokens // depth, clear, 0)

        def step(m, _):
            pass_on(0, m)
            turn(0, m - 1)

            @pl.when(m >= 3)
            def _():
                down(m - 3)
            fetch(0, m - 1)
            pass_on(1, m - 1)

            @pl.when(m >= 2)
            def _():
                turn(1, m - 2)
            up(m - 1)

            @pl.when(m >= 2)
            def _():
                fetch(1, m - 2)
            return 0

        lax.fori_loop(1, last, step, 0)
        pass_on(0, last)
        turn(0, last - 1)
        down(last - 3)
        fetch(0, last - 1)
        pass_late(0)
        turn(1, last - 2)
        up(last - 1)
        pass_late(1)
        fetch(1, last - 2)
        turn(0, last)
        pass_late(2)
        down(last - 2)
        pass_late(3)
        for q in range(4):
            turn_late(q)
        stale(0, last).wait()
        for m in range(last - 1, chunks):
            stale(1, m).wait()
        own(0, last, sib).wait_recv()
        next_own(0, last, sib_cross).wait_recv()

        def drain(m, _):
            across(0, m, rep).wait_send()
            own(0, m, rep).wait_send()
            next_own(0, m, cross).wait_send()

            @pl.when(m < last - 1)
            def _():
                across(1, m, rep).wait_send()
                own(1, m, rep).wait_send()
                next_own(1, m, cross).wait_send()
            return 0
        lax.fori_loop(0, chunks, drain, 0)
        for q in range(4):
            late_hop(q, sib, sib, ot_send, ot_recv).wait_recv()
            cross_hop(q, sib_cross, sib, nt_send, nt_recv).wait_recv()
        for q in range(4):
            if q < 3:
                cross_hop(q, rep, cross, xt_send, xt_recv).wait_send()
            late_hop(q, rep, sib, ot_send, ot_recv).wait_send()
            cross_hop(q, cross, sib, nt_send, nt_recv).wait_send()


def finish_kernel(x_v, acc, new_dn, u_v, sb_up, sb_dn, last_dn, zero, land_up, up_out, dn_out, y_out,
                  wg_up, wg, y_v, u_last, lb_up, sem, y_sem, l_sem):
    side = lax.axis_index("side")
    depth = acc.shape[0]
    tokens, width = x_v.shape
    n = up_out.shape[1] // width
    rows_dn = dn_out.shape[0] // n
    blocks = tokens // depth
    pieces = width // zero.shape[1]

    def up_piece(i):
        return pl.ds(i * width, width)

    def dn_piece(i):
        return pl.ds(i * rows_dn, rows_dn)

    def y_piece(i):
        return y_out.at[pl.ds(i * depth, depth), :]

    @pl.when(side == 0)
    def trainer():
        copies = []
        for i in range(n):
            copies.append(pltpu.make_async_copy(acc.at[:, up_piece(i)], up_out.at[:, up_piece(i)], sem.at[0, i, 0]))
            copies.append(pltpu.make_async_copy(new_dn.at[dn_piece(i), :], dn_out.at[dn_piece(i), :], sem.at[1, i, 0]))
        y_v[0] = jnp.zeros_like(y_v[0])
        for c in copies:
            c.start()
        ys = [pltpu.make_async_copy(y_v.at[0], y_piece(i), y_sem.at[i]) for i in range(blocks)]
        for c in ys:
            c.start()
        for c in copies + ys:
            c.wait()

    @pl.when(side == 1)
    def generator():
        last = land_up.shape[0] - 1
        landed = pltpu.make_async_copy(land_up.at[last], lb_up, l_sem.at[0])
        landed.start()
        size = zero.shape[1]
        copies = []
        for i in range(n):
            for j in range(pieces):
                copies.append(pltpu.make_async_copy(
                    zero, up_out.at[:, pl.ds(i * width + j * size, size)], sem.at[0, i, j]))
                copies.append(pltpu.make_async_copy(
                    zero, dn_out.at[pl.ds(i * rows_dn + j * depth, depth), :], sem.at[1, i, j]))
        for c in copies:
            c.start()
        for k in range(2):
            ks = pl.ds(k * COLS, COLS)
            for r in range(4):
                cols = pl.ds(r * depth, depth)
                wg[ks, cols] = (sb_dn[k, :, cols].astype(jnp.float32) + last_dn[r, ks, :].astype(jnp.float32)).astype(jnp.bfloat16)
        landed.wait()
        for r in range(4):
            rows = pl.ds(r * depth, depth)
            wg_up[rows, :] = (sb_up[last % 2, rows, :].astype(jnp.float32) + lb_up[r].astype(jnp.float32)).astype(jnp.bfloat16)

        def up(i, _):
            rows = pl.ds(pl.multiple_of(i * TILE, TILE), TILE)
            pre = jnp.dot(x_v[rows, :], wg_up[...], preferred_element_type=jnp.float32)
            u_last[rows, :] = gelu(pre).astype(jnp.bfloat16)
            return 0
        lax.fori_loop(0, tokens // TILE, up, 0)

        def out(i):
            return pltpu.make_async_copy(y_v.at[i], y_out.at[pl.ds(pl.multiple_of(i * depth, depth), depth), :], y_sem.at[i])

        def block(i, _):
            rows = pl.ds(pl.multiple_of(i * depth, depth), depth)
            cols = pl.ds(pl.multiple_of(i * width, width), width)
            u = jnp.concatenate([u_v[rows, :COLS], u_last[rows, :]], axis=1)
            p = jnp.dot(u, wg[...], preferred_element_type=jnp.float32)
            y_v[i] = (acc[:, cols] + p).astype(jnp.bfloat16)

            @pl.when(i >= 1)
            def _():
                out(i - 1).start()
            return 0
        lax.fori_loop(0, blocks, block, 0)
        for c in copies[:len(copies) // 2]:
            c.wait()
        out(blocks - 1).start()
        for c in copies[len(copies) // 2:]:
            c.wait()
        for i in range(blocks):
            out(i).wait()


def step_outputs(lr, w_up, w_dn, g_up, g_dn, s_up, s_dn, x):
    depth, hid = w_up.shape
    tokens, width = x.shape
    chunks = hid // COLS
    any_spec = pl.BlockSpec(memory_space=pltpu.HBM)
    vmem_spec = pl.BlockSpec(memory_space=pltpu.VMEM)
    dma = pltpu.SemaphoreType.DMA
    vmem = pltpu.VMEM
    f32, bf16 = jnp.float32, jnp.bfloat16
    land_up, _, *held = pl.pallas_call(
        sync_kernel,
        name="sync_kernel",
        out_shape=(
            jax.ShapeDtypeStruct((chunks, 4, depth, COLS), bf16),
            jax.ShapeDtypeStruct((chunks, 4, COLS, depth), bf16),
            vmem((tokens, width), bf16),
            vmem(w_up.shape, f32),
            vmem(w_dn.shape, f32),
            vmem((tokens, 2 * COLS), bf16),
            vmem((2, width, COLS), bf16),
            vmem((2, COLS, width), bf16),
            vmem((4, 2 * COLS, depth), bf16),
            vmem((depth, depth), f32),
        ),
        in_specs=[any_spec] * 8,
        out_specs=(any_spec,) * 2 + (vmem_spec,) * 8,
        scratch_shapes=[
            vmem((2, depth, COLS), f32), vmem((2, COLS, depth), f32),
            vmem((2, depth, COLS), f32), vmem((2, COLS, depth), f32),
            vmem((SENDS, depth, COLS), bf16), vmem((SENDS, COLS, depth), bf16),
            vmem((SWAP, depth), bf16),
            vmem((4, depth, COLS), bf16), vmem((4, COLS, depth), bf16),
            vmem((width, COLS), bf16), vmem((COLS, width), bf16),
            pltpu.SMEM((1,), f32), dma((4, 2)), dma((2, SENDS)), dma((2, 2)), dma((2,)), dma((1,)),
        ] + [dma((2, chunks))] * 7 + [dma((5,))] * 7 + [dma((2,))],
        compiler_params=pltpu.CompilerParams(
            collective_id=0, has_side_effects=True, vmem_limit_bytes=VMEM_SYNC),
        cost_estimate=pl.CostEstimate(flops=4 * tokens * width * hid, bytes_accessed=8 * width * hid, transcendentals=0),
    )(lr, w_up, w_dn, g_up, g_dn, s_up, s_dn, x)
    n = hid // width
    return pl.pallas_call(
        finish_kernel,
        name="finish_kernel",
        out_shape=(
            jax.ShapeDtypeStruct(w_up.shape, f32),
            jax.ShapeDtypeStruct(w_dn.shape, f32),
            jax.ShapeDtypeStruct((tokens, width), bf16),
        ),
        in_specs=[vmem_spec] * 8 + [any_spec],
        out_specs=(any_spec,) * 3,
        scratch_shapes=[
            vmem((width, COLS), bf16), vmem((2 * COLS, width), bf16),
            vmem((tokens // depth, depth, width), bf16),
            vmem((tokens, COLS), bf16), vmem((4, depth, COLS), bf16),
            dma((2, n, width // depth)), dma((tokens // depth,)), dma((1,)),
        ],
        compiler_params=pltpu.CompilerParams(vmem_limit_bytes=VMEM_FINISH),
        cost_estimate=pl.CostEstimate(flops=4 * tokens * width * COLS, bytes_accessed=12 * depth * hid, transcendentals=0),
    )(*[pltpu.with_memory_space_constraint(a, pltpu.VMEM) for a in held], land_up)


def solution(mesh):
    up_spec = P("side", None, "rep", None)
    down_spec = P("side", None, None, "rep")
    copy_spec = P("side", "rep", None, None, None)
    token_spec = P("side", "rep", None, None)

    def local_step(w_up, w_down, g_up, g_down, learn_rate, old_up, old_down, prompts):
        new_up, new_down, y = step_outputs(
            learn_rate, w_up[0, 0], w_down[0, 0], g_up[0, 0], g_down[0, 0],
            old_up[0, 0, 0], old_down[0, 0, 0], prompts[0, 0])
        return new_up[None, None], new_down[None, None], y[None, None]

    return jax.shard_map(
        local_step,
        mesh=mesh,
        in_specs=(up_spec, down_spec, up_spec, down_spec, P(None), copy_spec, copy_spec, token_spec),
        out_specs=(up_spec, down_spec, token_spec),
        check_vma=False,
    )
```

```python
import functools

import jax
import jax.numpy as jnp
from jax import lax
from jax.experimental import pallas as pl
from jax.experimental.pallas import tpu as pltpu
from jax.sharding import PartitionSpec as P

MESH = pl.DeviceIdType.MESH
COLS = 256
SENDS = 4
TILE = 1024
HALF = COLS // 2
SWAP = 160
VMEM_SYNC = 13 * 1024 * 1024
VMEM_FINISH = 13 * 1024 * 1024


def gelu(x):
    return 0.5 * x * (1.0 + lax.erf(x * 0.7071067811865476))


def sync_kernel(lr_hbm, w_up, w_dn, g_up, g_dn, s_up, s_dn, x_hbm,
                land_up, land_dn, x_v, acc, new_dn, u_v, sb_up, sb_dn, last_dn, zero, lb_up,
                wb_up, wb_dn, gb_up, gb_dn, d_up, d_dn, swap_dn, lb_dn, wg_up, wg_dn,
                lr, t_sem, send_sem, s_sem, l_sem, x_sem,
                y_recv, x_recv, o_recv, n_recv, x_send, o_send, n_send,
                yt_recv, xt_recv, ot_recv, nt_recv, xt_send, ot_send, nt_send, swap_sem):
    side, rep = lax.axis_index("side"), lax.axis_index("rep")
    other = 1 - side
    sib = rep + 1 - 2 * (rep % 2)
    cross = (rep + 2) % 4
    sib_cross = (sib + 2) % 4
    chunks = land_up.shape[0]
    depth = w_up.shape[0]
    tokens, width = x_v.shape
    lands, smalls = (land_up, land_dn), (d_up, d_dn)
    last = chunks - 1

    barrier = pltpu.get_barrier_semaphore()
    for dev in ((other, rep), (side, sib), (side, cross)):
        pl.semaphore_signal(barrier, inc=1, device_id=dev, device_id_type=MESH)

    def span(m):
        return pl.ds(pl.multiple_of(m * COLS, COLS), COLS)

    def swapped(row):
        return last_dn.at[row, pl.ds(2 * COLS - SWAP, SWAP), :]

    def late(row, q):
        return last_dn.at[row, pl.ds(q * HALF, HALF), :]

    @pl.when(side == 0)
    def trainer():
        mats = ((w_up, g_up, wb_up, gb_up), (w_dn, g_dn, wb_dn, gb_dn))

        def part(h, ref, m):
            return ref.at[:, span(m)] if h == 0 else ref.at[span(m), :]

        def loads(h, m):
            w, g, wb, gb = mats[h]
            k = m % 2
            return [
                pltpu.make_async_copy(part(h, w, m), wb.at[k], t_sem.at[2 * h, k]),
                pltpu.make_async_copy(part(h, g, m), gb.at[k], t_sem.at[2 * h + 1, k]),
            ]

        def send(h, m):
            return pltpu.make_async_remote_copy(
                src_ref=smalls[h].at[m % SENDS], dst_ref=lands[h].at[m, rep],
                send_sem=send_sem.at[h, m % SENDS], recv_sem=y_recv.at[h, m],
                device_id=(other, rep), device_id_type=MESH)

        def send_late(q):
            m = last - 1 + q // 2
            return pltpu.make_async_remote_copy(
                src_ref=d_dn.at[m % SENDS, pl.ds((q % 2) * HALF, HALF), :], dst_ref=late(rep, q),
                send_sem=xt_send.at[q], recv_sem=yt_recv.at[q],
                device_id=(other, rep), device_id_type=MESH)

        swap = pltpu.make_async_remote_copy(
            src_ref=d_dn.at[last % SENDS, pl.ds(COLS - SWAP, SWAP), :], dst_ref=swap_dn,
            send_sem=swap_sem.at[0], recv_sem=swap_sem.at[1],
            device_id=(side, cross), device_id_type=MESH)
        send_swapped = pltpu.make_async_remote_copy(
            src_ref=swap_dn, dst_ref=swapped(cross),
            send_sem=xt_send.at[4], recv_sem=yt_recv.at[4],
            device_id=(other, rep), device_id_type=MESH)

        lr_in = pltpu.make_async_copy(lr_hbm, lr, x_sem.at[0])
        lr_in.start()
        for c in loads(0, 0):
            c.start()
        lr_in.wait()
        rate = lr[0]

        def make(h, m):
            k = m % 2
            for c in loads(h, m):
                c.wait()

            @pl.when(m >= SENDS)
            def _():
                send(h, m - SENDS).wait_send()
            old = mats[h][2][k]
            new = old - rate * mats[h][3][k]
            if h == 0:
                acc[:, span(m)] = new
            else:
                new_dn[span(m), :] = new
            smalls[h][m % SENDS] = (new - old).astype(jnp.bfloat16)

            @pl.when(m + 2 < chunks)
            def _():
                for c in loads(h, m + 2):
                    c.start()

        make(0, 0)
        for h, m in ((0, 1), (1, 0), (1, 1)):
            for c in loads(h, m):
                c.start()
        pl.semaphore_wait(barrier, 3)
        send(0, 0).start()

        def step(m, _):
            make(0, m + 1)

            @pl.when(m >= 1)
            def _():
                send(1, m - 1).start()
            make(1, m)
            send(0, m + 1).start()
            return 0

        lax.fori_loop(0, last, step, 0)
        make(1, last)
        for q in range(4):
            send_late(q).start()
        for h in range(2):
            send(h, chunks - SENDS).wait_send()
        swap.start()
        swap.wait_recv()
        send_swapped.start()
        swap.wait_send()
        for m in range(chunks - SENDS + 1, chunks):
            send(0, m).wait_send()
        for m in range(chunks - SENDS + 1, last - 1):
            send(1, m).wait_send()
        for q in range(4):
            send_late(q).wait_send()
        send_swapped.wait_send()

    @pl.when(side == 1)
    def generator():
        def hop(h, m, row, dev, send, recv):
            return pltpu.make_async_remote_copy(
                src_ref=lands[h].at[m, row], dst_ref=lands[h].at[m, row],
                send_sem=send.at[h, m], recv_sem=recv.at[h, m],
                device_id=(side, dev), device_id_type=MESH)

        def from_trainer(h, m):
            return hop(h, m, rep, sib, x_send, y_recv)

        def across(h, m, row):
            return hop(h, m, row, cross, x_send, x_recv)

        def own(h, m, row):
            return hop(h, m, row, sib, o_send, o_recv)

        def next_own(h, m, row):
            return hop(h, m, row, sib, n_send, n_recv)

        def cross_part(q):
            first = q * HALF if q < 3 else 2 * COLS - SWAP
            return pl.ds(first, min(HALF, 2 * COLS - SWAP - first) if q < 3 else SWAP)

        def cross_hop(q, row, dev, send, recv):
            ref = last_dn.at[row, cross_part(q), :]
            return pltpu.make_async_remote_copy(
                src_ref=ref, dst_ref=ref, send_sem=send.at[q], recv_sem=recv.at[q],
                device_id=(side, dev), device_id_type=MESH)

        def late_hop(q, row, dev, send, recv):
            return pltpu.make_async_remote_copy(
                src_ref=late(row, q), dst_ref=late(row, q), send_sem=send.at[q], recv_sem=recv.at[q],
                device_id=(side, dev), device_id_type=MESH)

        stales = (sb_up, sb_dn)

        def stale(h, m):
            src = s_up.at[:, span(m)] if h == 0 else s_dn.at[span(m), :]
            return pltpu.make_async_copy(src, stales[h].at[m % 2], s_sem.at[h, m % 2])

        def landed(h, m):
            return pltpu.make_async_copy(lands[h].at[m], (lb_up, lb_dn)[h], l_sem.at[h])

        x_in = pltpu.make_async_copy(x_hbm, x_v, x_sem.at[0])
        x_in.start()
        for m in range(2):
            for h in range(2):
                stale(h, m).start()
        pl.semaphore_wait(barrier, 3)

        def pass_on(h, m):
            from_trainer(h, m).wait_recv()
            across(h, m, rep).start()
            own(h, m, rep).start()

        def pass_late(q):
            late_hop(q, rep, sib, xt_send, yt_recv).wait_recv()
            if q < 3:
                cross_hop(q, rep, cross, xt_send, xt_recv).start()
            late_hop(q, rep, sib, ot_send, ot_recv).start()

        def turn(h, m):
            across(h, m, cross).wait_recv()
            next_own(h, m, cross).start()

        def turn_late(q):
            if q < 3:
                cross_hop(q, cross, cross, xt_send, xt_recv).wait_recv()
            else:
                pltpu.make_async_remote_copy(
                    src_ref=swapped(cross), dst_ref=swapped(cross), send_sem=xt_send.at[4], recv_sem=yt_recv.at[4],
                    device_id=(side, sib), device_id_type=MESH).wait_recv()
            cross_hop(q, cross, sib, nt_send, nt_recv).start()

        def fetch(h, m):
            own(h, m, sib).wait_recv()
            next_own(h, m, sib_cross).wait_recv()
            landed(h, m).start()

        tiles = tokens // TILE
        groups = TILE // depth

        def tile_rows(i):
            return pl.ds(pl.multiple_of(i * TILE, TILE), TILE)

        def u_cols(m):
            return pl.ds(pl.multiple_of((m % 2) * COLS, COLS), COLS)

        def up(m):
            k = m % 2
            stale(0, m).wait()
            landed(0, m).wait()
            for r in range(4):
                rows = pl.ds(r * depth, depth)
                wg_up[rows, :] = (sb_up[k, rows, :].astype(jnp.float32) + lb_up[r].astype(jnp.float32)).astype(jnp.bfloat16)

            @pl.when(m + 2 < chunks)
            def _():
                stale(0, m + 2).start()

            def tile(i, _):
                pre = jnp.dot(x_v[tile_rows(i), :], wg_up[...], preferred_element_type=jnp.float32)
                u_v[tile_rows(i), u_cols(m)] = gelu(pre).astype(jnp.bfloat16)
                return 0
            lax.fori_loop(0, tiles, tile, 0)

        def down(m):
            k = m % 2
            stale(1, m).wait()
            landed(1, m).wait()
            for r in range(4):
                cols = pl.ds(r * depth, depth)
                wg_dn[:, cols] = (sb_dn[k, :, cols].astype(jnp.float32) + lb_dn[r].astype(jnp.float32)).astype(jnp.bfloat16)

            @pl.when(m + 2 < chunks)
            def _():
                stale(1, m + 2).start()

            def tile(i, _):
                p = jnp.dot(u_v[tile_rows(i), u_cols(m)], wg_dn[...], preferred_element_type=jnp.float32)
                for g in range(groups):
                    cols = pl.ds(pl.multiple_of((i * groups + g) * width, width), width)
                    acc[:, cols] += p[g * depth:(g + 1) * depth]
                return 0
            lax.fori_loop(0, tiles, tile, 0)

        pass_on(0, 0)
        x_in.wait()
        zero[...] = jnp.zeros_like(zero)

        def clear(i, _):
            cols = pl.ds(pl.multiple_of(i * width, width), width)
            rows = pl.ds(pl.multiple_of(i * depth, depth), depth)
            acc[:, cols] = x_v[rows, :].astype(jnp.float32)
            return 0
        lax.fori_loop(0, tokens // depth, clear, 0)

        def step(m, _):
            pass_on(0, m)
            turn(0, m - 1)

            @pl.when(m >= 3)
            def _():
                down(m - 3)
            fetch(0, m - 1)
            pass_on(1, m - 1)

            @pl.when(m >= 2)
            def _():
                turn(1, m - 2)
            up(m - 1)

            @pl.when(m >= 2)
            def _():
                fetch(1, m - 2)
            return 0

        lax.fori_loop(1, last, step, 0)
        pass_on(0, last)
        turn(0, last - 1)
        down(last - 3)
        fetch(0, last - 1)
        pass_late(0)
        turn(1, last - 2)
        up(last - 1)
        pass_late(1)
        fetch(1, last - 2)
        turn(0, last)
        pass_late(2)
        down(last - 2)
        pass_late(3)
        fetch(0, last)
        for q in range(4):
            turn_late(q)
        stale(0, last).wait()
        for m in range(last - 1, chunks):
            stale(1, m).wait()
        landed(0, last).wait()

        def drain(m, _):
            across(0, m, rep).wait_send()
            own(0, m, rep).wait_send()
            next_own(0, m, cross).wait_send()

            @pl.when(m < last - 1)
            def _():
                across(1, m, rep).wait_send()
                own(1, m, rep).wait_send()
                next_own(1, m, cross).wait_send()
            return 0
        lax.fori_loop(0, chunks, drain, 0)
        for q in range(4):
            late_hop(q, sib, sib, ot_send, ot_recv).wait_recv()
            cross_hop(q, sib_cross, sib, nt_send, nt_recv).wait_recv()
        for q in range(4):
            if q < 3:
                cross_hop(q, rep, cross, xt_send, xt_recv).wait_send()
            late_hop(q, rep, sib, ot_send, ot_recv).wait_send()
            cross_hop(q, cross, sib, nt_send, nt_recv).wait_send()


def finish_kernel(x_v, acc, new_dn, u_v, sb_up, sb_dn, last_dn, zero, lb_up, up_out, dn_out, y_out,
                  wg_up, wg, y_v, u_last, sem, y_sem):
    side = lax.axis_index("side")
    depth = acc.shape[0]
    tokens, width = x_v.shape
    n = up_out.shape[1] // width
    rows_dn = dn_out.shape[0] // n
    blocks = tokens // depth
    pieces = width // zero.shape[1]

    def up_piece(i):
        return pl.ds(i * width, width)

    def dn_piece(i):
        return pl.ds(i * rows_dn, rows_dn)

    def y_piece(i):
        return y_out.at[pl.ds(i * depth, depth), :]

    @pl.when(side == 0)
    def trainer():
        copies = []
        for i in range(n):
            copies.append(pltpu.make_async_copy(acc.at[:, up_piece(i)], up_out.at[:, up_piece(i)], sem.at[0, i, 0]))
            copies.append(pltpu.make_async_copy(new_dn.at[dn_piece(i), :], dn_out.at[dn_piece(i), :], sem.at[1, i, 0]))
        y_v[0] = jnp.zeros_like(y_v[0])
        for c in copies:
            c.start()
        ys = [pltpu.make_async_copy(y_v.at[0], y_piece(i), y_sem.at[i]) for i in range(blocks)]
        for c in ys:
            c.start()
        for c in copies + ys:
            c.wait()

    @pl.when(side == 1)
    def generator():
        size = zero.shape[1]
        copies = []
        for i in range(n):
            for j in range(pieces):
                copies.append(pltpu.make_async_copy(
                    zero, up_out.at[:, pl.ds(i * width + j * size, size)], sem.at[0, i, j]))
                copies.append(pltpu.make_async_copy(
                    zero, dn_out.at[pl.ds(i * rows_dn + j * depth, depth), :], sem.at[1, i, j]))
        for c in copies:
            c.start()
        for k in range(2):
            ks = pl.ds(k * COLS, COLS)
            for r in range(4):
                cols = pl.ds(r * depth, depth)
                wg[ks, cols] = (sb_dn[k, :, cols].astype(jnp.float32) + last_dn[r, ks, :].astype(jnp.float32)).astype(jnp.bfloat16)
        for r in range(4):
            rows = pl.ds(r * depth, depth)
            wg_up[rows, :] = (sb_up[1, rows, :].astype(jnp.float32) + lb_up[r].astype(jnp.float32)).astype(jnp.bfloat16)

        def up(i, _):
            rows = pl.ds(pl.multiple_of(i * TILE, TILE), TILE)
            pre = jnp.dot(x_v[rows, :], wg_up[...], preferred_element_type=jnp.float32)
            u_last[rows, :] = gelu(pre).astype(jnp.bfloat16)
            return 0
        lax.fori_loop(0, tokens // TILE, up, 0)

        def out(i):
            return pltpu.make_async_copy(y_v.at[i], y_out.at[pl.ds(pl.multiple_of(i * depth, depth), depth), :], y_sem.at[i])

        def block(i, _):
            rows = pl.ds(pl.multiple_of(i * depth, depth), depth)
            cols = pl.ds(pl.multiple_of(i * width, width), width)
            u = jnp.concatenate([u_v[rows, :COLS], u_last[rows, :]], axis=1)
            p = jnp.dot(u, wg[...], preferred_element_type=jnp.float32)
            y_v[i] = (acc[:, cols] + p).astype(jnp.bfloat16)

            @pl.when(i >= 1)
            def _():
                out(i - 1).start()
            return 0
        lax.fori_loop(0, blocks, block, 0)
        for c in copies[:len(copies) // 2]:
            c.wait()
        out(blocks - 1).start()
        for c in copies[len(copies) // 2:]:
            c.wait()
        for i in range(blocks):
            out(i).wait()


def step_outputs(lr, w_up, w_dn, g_up, g_dn, s_up, s_dn, x):
    depth, hid = w_up.shape
    tokens, width = x.shape
    chunks = hid // COLS
    any_spec = pl.BlockSpec(memory_space=pltpu.HBM)
    vmem_spec = pl.BlockSpec(memory_space=pltpu.VMEM)
    dma = pltpu.SemaphoreType.DMA
    vmem = pltpu.VMEM
    f32, bf16 = jnp.float32, jnp.bfloat16
    _, _, *held = pl.pallas_call(
        sync_kernel,
        name="sync_kernel",
        out_shape=(
            jax.ShapeDtypeStruct((chunks, 4, depth, COLS), bf16),
            jax.ShapeDtypeStruct((chunks, 4, COLS, depth), bf16),
            vmem((tokens, width), bf16),
            vmem(w_up.shape, f32),
            vmem(w_dn.shape, f32),
            vmem((tokens, 2 * COLS), bf16),
            vmem((2, width, COLS), bf16),
            vmem((2, COLS, width), bf16),
            vmem((4, 2 * COLS, depth), bf16),
            vmem((depth, depth), f32),
            vmem((4, depth, COLS), bf16),
        ),
        in_specs=[any_spec] * 8,
        out_specs=(any_spec,) * 2 + (vmem_spec,) * 9,
        scratch_shapes=[
            vmem((2, depth, COLS), f32), vmem((2, COLS, depth), f32),
            vmem((2, depth, COLS), f32), vmem((2, COLS, depth), f32),
            vmem((SENDS, depth, COLS), bf16), vmem((SENDS, COLS, depth), bf16),
            vmem((SWAP, depth), bf16),
            vmem((4, COLS, depth), bf16),
            vmem((width, COLS), bf16), vmem((COLS, width), bf16),
            pltpu.SMEM((1,), f32), dma((4, 2)), dma((2, SENDS)), dma((2, 2)), dma((2,)), dma((1,)),
        ] + [dma((2, chunks))] * 7 + [dma((5,))] * 7 + [dma((2,))],
        compiler_params=pltpu.CompilerParams(
            collective_id=0, has_side_effects=True, vmem_limit_bytes=VMEM_SYNC),
        cost_estimate=pl.CostEstimate(flops=4 * tokens * width * hid, bytes_accessed=8 * width * hid, transcendentals=0),
    )(lr, w_up, w_dn, g_up, g_dn, s_up, s_dn, x)
    n = hid // width
    return pl.pallas_call(
        finish_kernel,
        name="finish_kernel",
        out_shape=(
            jax.ShapeDtypeStruct(w_up.shape, f32),
            jax.ShapeDtypeStruct(w_dn.shape, f32),
            jax.ShapeDtypeStruct((tokens, width), bf16),
        ),
        in_specs=[vmem_spec] * 9,
        out_specs=(any_spec,) * 3,
        scratch_shapes=[
            vmem((width, COLS), bf16), vmem((2 * COLS, width), bf16),
            vmem((tokens // depth, depth, width), bf16),
            vmem((tokens, COLS), bf16),
            dma((2, n, width // depth)), dma((tokens // depth,)),
        ],
        compiler_params=pltpu.CompilerParams(vmem_limit_bytes=VMEM_FINISH),
        cost_estimate=pl.CostEstimate(flops=4 * tokens * width * COLS, bytes_accessed=12 * depth * hid, transcendentals=0),
    )(*[pltpu.with_memory_space_constraint(a, pltpu.VMEM) for a in held])


def solution(mesh):
    up_spec = P("side", None, "rep", None)
    down_spec = P("side", None, None, "rep")
    copy_spec = P("side", "rep", None, None, None)
    token_spec = P("side", "rep", None, None)

    def local_step(w_up, w_down, g_up, g_down, learn_rate, old_up, old_down, prompts):
        new_up, new_down, y = step_outputs(
            learn_rate, w_up[0, 0], w_down[0, 0], g_up[0, 0], g_down[0, 0],
            old_up[0, 0, 0], old_down[0, 0, 0], prompts[0, 0])
        return new_up[None, None], new_down[None, None], y[None, None]

    return jax.shard_map(
        local_step,
        mesh=mesh,
        in_specs=(up_spec, down_spec, up_spec, down_spec, P(None), copy_spec, copy_spec, token_spec),
        out_specs=(up_spec, down_spec, token_spec),
        check_vma=False,
    )
```
